256 devices in a mesh: row: 8 (over z_hi, y), col: 32 (over z_lo, x, core).
Axes of the slice: x: 4, y: 4, z: 8 (z_hi: 2, z_lo: 4; z = z_hi * 4 + z_lo), core: 2. Of those that a mesh axis runs over, the one named last changes fastest.
Arguments:
- tokens: bfloat16 [4096, 1024], P(('row', 'col')), may hold values from -6 to 6
- grad_out: bfloat16 [4096, 1024], P(('row', 'col')), may hold values from -1.1953125 to 1.1953125
- gains: float32 [2, 1024], replicated, may hold values from 0.1 to 1.9
- flat_in: bfloat16 [32768, 1024], P(('row', 'col')), may hold values from -0.1875 to 0.1875
- flat_out: bfloat16 [32768, 1024], P(('row', 'col')), may hold values from -0.03125 to 0.03125
- flat_moment: float32 [2, 32768, 1024], P(None, ('row', 'col')), may hold values from -3 to 3
- flat_second: float32 [2, 32768, 1024], P(None, ('row', 'col')), may hold values from 0.05 to 2
- tile_in: bfloat16 [32, 24, 64, 1024], P('col', 'row'), may hold values from -0.1875 to 0.1875
- tile_out: bfloat16 [32, 24, 64, 1024], P('col', 'row'), may hold values from -0.03125 to 0.03125
- tile_moment: float32 [2, 32, 24, 64, 1024], P(None, 'col', 'row'), may hold values from -3 to 3
- tile_second: float32 [2, 32, 24, 64, 1024], P(None, 'col', 'row'), may hold values from 0.05 to 2
- owners: int32 [2, 32, 16], P(None, 'col'), may hold values from 0 to 7, as said below
Outputs:
- hidden_out: bfloat16 [4096, 1024], P(('row', 'col'))
- grad_tokens: bfloat16 [4096, 1024], P(('row', 'col'))
- new_flat_in: bfloat16 [32768, 1024], P(('row', 'col'))
- new_flat_out: bfloat16 [32768, 1024], P(('row', 'col'))
- new_flat_moment: float32 [2, 32768, 1024], P(None, ('row', 'col'))
- new_flat_second: float32 [2, 32768, 1024], P(None, ('row', 'col'))
- new_tile_in: bfloat16 [32, 24, 64, 1024], P('col', 'row')
- new_tile_out: bfloat16 [32, 24, 64, 1024], P('col', 'row')
- new_tile_moment: float32 [2, 32, 24, 64, 1024], P(None, 'col', 'row')
- new_tile_second: float32 [2, 32, 24, 64, 1024], P(None, 'col', 'row')
The draws below stay inside these ranges and needn't reach their ends.
Inputs may be any that keep to these rules, and one draw needn't show every extreme that they name: `owners`: for each matrix and column block, entry k names the row that owns tile k; each row owns at most 3 tiles of a block and matrix, and in each block and matrix some row owns exactly 3.
All inputs are finite; a program needn't handle non-finite values.
Results may differ from the reference program's by a relative error of at most 0.029.
Values may be sent and summed in bfloat16 or wider, within the bound.
A program may use at most 128 MiB of HBM per device.

```python
import math
import jax
import jax.numpy as jnp
from jax import lax

D = 1024
FF = 32768
OWN_CAP = 3
TOKENS = 4096
GROUP_TOK = 512
BLOCK = 1024
TILES = 16
TILE_ROWS = 64
N_ROW = 8
N_COL = 32


def draw_owners(key, part):
    owner_pool = jnp.repeat(jnp.arange(N_ROW, dtype=jnp.int32), OWN_CAP)

    def one_block(sub_key):
        key_full, key_pick, key_order = jax.random.split(sub_key, 3)
        favored = jax.random.randint(key_full, (), 0, N_ROW, dtype=jnp.int32)
        scores = jax.random.permutation(key_pick, N_ROW * OWN_CAP).astype(jnp.int32) + jnp.where(owner_pool == favored, N_ROW * OWN_CAP, 0).astype(jnp.int32)
        picked = jnp.argsort(-scores, stable=True)[:2 * N_ROW]
        chosen = owner_pool[picked]
        return chosen[jax.random.permutation(key_order, 2 * N_ROW)]
    block_keys = jax.random.split(jax.random.fold_in(key, 17), 2 * N_COL)
    return jax.vmap(one_block)(block_keys).reshape(2, N_COL, 2 * N_ROW).astype(jnp.int32)


def block_levels(own_key, dims, cuts, least, high):
    factor_of, own = 1.0, jax.random.fold_in(own_key, 6)
    for position, shards_of in cuts:
        draws = jnp.exp(jax.random.uniform(jax.random.fold_in(own, position), (shards_of,), jnp.float32, least / len(cuts), high / len(cuts)))
        factor_of = factor_of * jnp.repeat(draws, dims[position] // shards_of).reshape([-1 if axis == position else 1 for axis in range(len(dims))])
    return factor_of


def bell_draw(rng, dims, deviation, reach, cuts=(), kind=jnp.bfloat16):
    drawn = jax.random.normal(rng, dims, jnp.float32) * deviation
    if len(cuts) > 0:
        drawn = block_levels(rng, dims, cuts, -0.22, 0.18) * drawn
    return jnp.clip(drawn, min=-reach, max=reach).astype(kind)


def setup_inputs(seed: int = 0) -> dict:
    streams_of = jax.random.split(jax.random.key(seed), 13)
    tokens = bell_draw(streams_of[0], (TOKENS, D), 1.0, 6.0, ((0, 256),))
    grad_out = bell_draw(streams_of[1], (TOKENS, D), 0.2, 1.1953125, ((0, 256),))
    gains = jnp.clip(1.0 + 0.18 * jax.random.normal(streams_of[2], (2, D), jnp.float32), 0.1, 1.9)
    flat_in = bell_draw(streams_of[3], (D * N_COL, BLOCK), D ** -0.5, 0.1875, ((0, 256),))
    flat_out = bell_draw(streams_of[4], (D * N_COL, BLOCK), FF ** -0.5, 0.03125, ((0, 256),))
    flat_moment = bell_draw(streams_of[5], (2, D * N_COL, BLOCK), 0.5, 3.0, ((1, 256),), jnp.float32)
    flat_second = jnp.clip(jnp.exp(math.log(2.0) - 3.6888794 * jax.random.uniform(streams_of[6], (2, D * N_COL, BLOCK), jnp.float32) ** block_levels(streams_of[6], (2, D * N_COL, BLOCK), ((1, 256),), -0.2, 0.2)), 0.05, 2.0)
    tile_in = bell_draw(streams_of[7], (N_COL, N_ROW * OWN_CAP, TILE_ROWS, BLOCK), D ** -0.5, 0.1875, ((0, 32), (1, 8)))
    tile_out = bell_draw(streams_of[8], (N_COL, N_ROW * OWN_CAP, TILE_ROWS, BLOCK), FF ** -0.5, 0.03125, ((0, 32), (1, 8)))
    tile_moment = bell_draw(streams_of[9], (2, N_COL, N_ROW * OWN_CAP, TILE_ROWS, BLOCK), 0.5, 3.0, ((1, 32), (2, 8)), jnp.float32)
    tile_second = jnp.clip(jnp.exp(math.log(2.0) - 3.6888794 * jax.random.uniform(streams_of[10], (2, N_COL, N_ROW * OWN_CAP, TILE_ROWS, BLOCK), jnp.float32) ** block_levels(streams_of[10], (2, N_COL, N_ROW * OWN_CAP, TILE_ROWS, BLOCK), ((1, 32), (2, 8)), -0.2, 0.2)), 0.05, 2.0)
    owners = draw_owners(jax.random.fold_in(streams_of[12], 71), 0)
    return dict(tokens=tokens, grad_out=grad_out, gains=gains, flat_in=flat_in, flat_out=flat_out, flat_moment=flat_moment, flat_second=flat_second, tile_in=tile_in, tile_out=tile_out, tile_moment=tile_moment, tile_second=tile_second, owners=owners)


norm_eps = 1e-06
beta_one = 0.9
beta_two = 0.95
learn_rate = 0.002
decay_rate = 0.1
adam_eps = 1e-08
gelu_coef = 0.7978845608

def gelu_value(hidden):
    tanh_term = jnp.tanh(gelu_coef * (hidden + 0.044715 * hidden * hidden * hidden))
    return 0.5 * hidden * (1.0 + tanh_term)

def gelu_slope(hidden):
    tanh_term = jnp.tanh(gelu_coef * (hidden + 0.044715 * hidden * hidden * hidden))
    return 0.5 * (1.0 + tanh_term) + 0.5 * hidden * (1.0 - tanh_term * tanh_term) * gelu_coef * (1.0 + 0.134145 * hidden * hidden)

def adam_update(weight, gradient, moment, second):
    new_moment = beta_one * moment + (1.0 - beta_one) * gradient
    new_second = beta_two * second + (1.0 - beta_two) * gradient * gradient
    weight_float = weight.astype(jnp.float32)
    stepped = weight_float - learn_rate * (new_moment / (jnp.sqrt(new_second) + adam_eps) + decay_rate * weight_float)
    return (stepped.astype(jnp.bfloat16), new_moment, new_second)

def slot_tables(owner_rows, slot_cap, row_total):
    tile_count = owner_rows.shape[-1]
    positions = jnp.arange(tile_count, dtype=jnp.int32)
    same_owner = owner_rows[..., :, None] == owner_rows[..., None, :]
    earlier = positions[None, :] < positions[:, None]
    tile_rank = lax.optimization_barrier(jnp.sum(jnp.where(same_owner & earlier, 1, 0), axis=-1)).astype(jnp.int32)
    slot_dest = (owner_rows * slot_cap + tile_rank).astype(jnp.int32)
    slot_ids = jnp.arange(row_total * slot_cap, dtype=jnp.int32)
    matches = slot_dest[..., None, :] == slot_ids[:, None]
    slot_tile = lax.optimization_barrier(jnp.sum(jnp.where(matches, positions, 0), axis=-1)).astype(jnp.int32)
    slot_live = jnp.any(matches, axis=-1)
    return (slot_dest, slot_tile, slot_live)

def layer_forward(layer_in, gain_vec, w_in, w_out):
    tok_float = layer_in.astype(jnp.float32)
    inv_rms = lax.rsqrt(lax.optimization_barrier(jnp.mean(tok_float * tok_float, axis=1, keepdims=True)) + norm_eps)
    normed = (tok_float * inv_rms * gain_vec).astype(jnp.bfloat16)
    hidden = jnp.dot(normed, w_in, preferred_element_type=jnp.float32)
    activated = gelu_value(hidden).astype(jnp.bfloat16)
    mixed_sum = lax.dot_general(activated, w_out, (((1,), (1,)), ((), ())), preferred_element_type=jnp.float32)
    return ((tok_float + mixed_sum).astype(jnp.bfloat16), (tok_float, inv_rms, normed, hidden, activated))

def group_sums(left_rows, right_rows):
    left_groups = left_rows.reshape(N_ROW, GROUP_TOK, left_rows.shape[1])
    right_groups = right_rows.reshape(N_ROW, GROUP_TOK, right_rows.shape[1])

    def add_group(running, operands):
        product = lax.dot_general(operands[0], operands[1], (((0,), (0,)), ((), ())), preferred_element_type=jnp.float32)
        rounded = lax.optimization_barrier(product.astype(jnp.bfloat16))
        return (running + rounded.astype(jnp.float32), None)
    start_sum = jnp.zeros((left_rows.shape[1], right_rows.shape[1]), jnp.float32)
    running, unused = lax.scan(add_group, start_sum, (left_groups, right_groups))
    return running

def layer_backward(cotangent, gain_vec, w_in, w_out, saved_state):
    tok_float, inv_rms, normed, hidden, activated = saved_state
    d_act = jnp.dot(cotangent, w_out, preferred_element_type=jnp.float32)
    d_hidden = (d_act * gelu_slope(hidden)).astype(jnp.bfloat16)
    d_normed = lax.dot_general(d_hidden, w_in, (((1,), (1,)), ((), ())), preferred_element_type=jnp.float32)
    gated = d_normed * gain_vec
    tok_grad = cotangent.astype(jnp.float32) + inv_rms * gated - tok_float * inv_rms * inv_rms * inv_rms * lax.optimization_barrier(jnp.mean(tok_float * gated, axis=1, keepdims=True))
    grad_in = group_sums(normed, d_hidden)
    grad_wout = group_sums(cotangent, activated)
    return (tok_grad.astype(jnp.bfloat16), grad_in, grad_wout)

def assemble(slot_data, slot_dest_m):
    tile_data = jnp.take_along_axis(slot_data, slot_dest_m[:, :, None, None], axis=1)
    return tile_data.transpose(1, 2, 0, 3).reshape(D, FF)

def tiled_update(slot_data, gradient, moment, second, slot_tile_m, slot_live_m):
    grad_tiles = gradient.reshape(TILES, TILE_ROWS, N_COL, BLOCK).transpose(2, 0, 1, 3)
    grad_slots = jnp.take_along_axis(grad_tiles, slot_tile_m[:, :, None, None], axis=1)
    new_weight, new_moment, new_second = adam_update(slot_data, grad_slots, moment, second)
    live_mask = slot_live_m[:, :, None, None]
    return (jnp.where(live_mask, new_weight, slot_data), jnp.where(live_mask, new_moment, moment), jnp.where(live_mask, new_second, second))

def reference(tokens, grad_out, gains, flat_in, flat_out, flat_moment, flat_second, tile_in, tile_out, tile_moment, tile_second, owners):
    slot_dest, slot_tile, slot_live = slot_tables(owners, OWN_CAP, N_ROW)
    first_in = flat_in.reshape(D, FF)
    first_out = flat_out.reshape(D, FF)
    second_in = assemble(tile_in, slot_dest[0])
    second_out = assemble(tile_out, slot_dest[1])
    middle, saved_one = layer_forward(tokens, gains[0], first_in, first_out)
    hidden_out, saved_two = layer_forward(middle, gains[1], second_in, second_out)
    grad_mid, grad_in_two, grad_out_two = layer_backward(grad_out, gains[1], second_in, second_out, saved_two)
    grad_tokens, grad_in_one, grad_out_one = layer_backward(grad_mid, gains[0], first_in, first_out, saved_one)
    new_flat_in, moment_in, second_in_f = adam_update(flat_in, grad_in_one.reshape(D * N_COL, BLOCK), flat_moment[0], flat_second[0])
    new_flat_out, moment_out, second_out_f = adam_update(flat_out, grad_out_one.reshape(D * N_COL, BLOCK), flat_moment[1], flat_second[1])
    new_tile_in, tmoment_in, tsecond_in = tiled_update(tile_in, grad_in_two, tile_moment[0], tile_second[0], slot_tile[0], slot_live[0])
    new_tile_out, tmoment_out, tsecond_out = tiled_update(tile_out, grad_out_two, tile_moment[1], tile_second[1], slot_tile[1], slot_live[1])
    return (hidden_out, grad_tokens, new_flat_in, new_flat_out, jnp.stack([moment_in, moment_out]), jnp.stack([second_in_f, second_out_f]), new_tile_in, new_tile_out, jnp.stack([tmoment_in, tmoment_out]), jnp.stack([tsecond_in, tsecond_out]))
```

```python
import functools

import jax
import jax.numpy as jnp
from jax import lax
from jax.experimental import pallas as pl
from jax.experimental.pallas import tpu as pltpu
from jax.sharding import Mesh, PartitionSpec as P

norm_eps = 1e-06
beta_one = 0.9
beta_two = 0.95
learn_rate = 0.002
decay_rate = 0.1
adam_eps = 1e-08
gelu_coef = 0.7978845608

ALL = ("zh", "y", "zl", "x", "c")
ROW = ("zh", "y")
COL = ("zl", "x", "c")
MESH = pl.DeviceIdType.MESH
BF = jnp.bfloat16
F32 = jnp.float32

def gelu_value(hidden):
    tanh_term = jnp.tanh(gelu_coef * (hidden + 0.044715 * hidden * hidden * hidden))
    return 0.5 * hidden * (1.0 + tanh_term)


def gelu_slope(hidden):
    tanh_term = jnp.tanh(gelu_coef * (hidden + 0.044715 * hidden * hidden * hidden))
    return 0.5 * (1.0 + tanh_term) + 0.5 * hidden * (1.0 - tanh_term * tanh_term) * gelu_coef * (
        1.0 + 0.134145 * hidden * hidden
    )


def adam_update(weight, gradient, moment, second):
    new_moment = beta_one * moment + (1.0 - beta_one) * gradient
    new_second = beta_two * second + (1.0 - beta_two) * gradient * gradient
    weight_float = weight.astype(jnp.float32)
    stepped = weight_float - learn_rate * (
        new_moment / (jnp.sqrt(new_second) + adam_eps) + decay_rate * weight_float
    )
    return (stepped.astype(jnp.bfloat16), new_moment, new_second)


def slot_tables(owner_rows, slot_cap, row_total):
    tile_count = owner_rows.shape[-1]
    positions = jnp.arange(tile_count, dtype=jnp.int32)
    same_owner = owner_rows[..., :, None] == owner_rows[..., None, :]
    earlier = positions[None, :] < positions[:, None]
    tile_rank = jnp.sum(jnp.where(same_owner & earlier, 1, 0), axis=-1).astype(jnp.int32)
    slot_dest = owner_rows * slot_cap + tile_rank
    slot_ids = jnp.arange(row_total * slot_cap, dtype=jnp.int32)
    matches = slot_dest[..., None, :] == slot_ids[:, None]
    slot_tile = jnp.sum(jnp.where(matches, positions, 0), axis=-1)
    slot_live = jnp.any(matches, axis=-1)
    return (slot_dest, slot_tile, slot_live)


def dev_z(z):
    return {"zh": z // 4, "zl": z % 4}


def at(a):
    return lax.axis_index(a)


def place():
    return at("zh") * 4 + at("zl"), at("x"), at("c"), at("y")


def peers_near(with_y):
    z, x, c, y = place()
    peers = [dev_z((z + d) % 8) for d in range(1, 8)]
    peers += [{"x": (x + 1) % 4}, {"x": (x + 3) % 4}, {"c": 1 - c}]
    if with_y:
        peers += [{"y": (y + 1) % 4}, {"y": (y + 3) % 4}]
    return peers


def greet(peers):
    sem = pltpu.get_barrier_semaphore()
    for p in peers:
        pl.semaphore_signal(sem, inc=1, device_id=p, device_id_type=MESH)
    pl.semaphore_wait(sem, len(peers))


def flat_dev(t):
    return {"zh": t // 32, "zl": (t // 8) % 4, "x": (t // 2) % 4, "c": t % 2}


def my_flat():
    z, x, c, _ = place()
    return z * 8 + x * 2 + c


def greet_all():
    me = my_flat()
    y = at("y")
    sem = pltpu.get_barrier_semaphore()

    def one(o, _):
        pl.semaphore_signal(sem, inc=1, device_id=flat_dev((me + o) % 64), device_id_type=MESH)
        return 0

    lax.fori_loop(1, 64, one, 0)
    for d in (1, 3):
        pl.semaphore_signal(sem, inc=1, device_id={"y": (y + d) % 4}, device_id_type=MESH)
    pl.semaphore_wait(sem, 65)


def rcopy(src, dst, ssem, rsem, dev):
    cp = pltpu.make_async_remote_copy(
        src_ref=src, dst_ref=dst, send_sem=ssem, recv_sem=rsem, device_id=dev, device_id_type=MESH
    )
    cp.start()
    return cp


def exchange_start(sbuf, rbuf, ssem, rsem):
    me = my_flat()

    def one(o, _):
        t = (me + o) % 64
        rcopy(sbuf.at[t], rbuf.at[me], ssem, rsem, flat_dev(t))
        return 0

    lax.fori_loop(1, 64, one, 0)
    rbuf[me] = sbuf[me]


def exchange_wait(sbuf, rbuf, ssem, rsem):
    part = pltpu.make_async_copy(rbuf.at[pl.ds(0, 63)], rbuf.at[pl.ds(0, 63)], rsem)
    part.wait()


def exchange_sent(sbuf, ssem):
    part = pltpu.make_async_copy(sbuf.at[pl.ds(0, 63)], sbuf.at[pl.ds(0, 63)], ssem)
    part.wait()


def blk(c, x, n=128, off=0):
    return pl.ds(pl.multiple_of(c * 512 + x * 128 + off, 16), n)


class Gather:
    sems = 7 + 2 + 2 + 4

    def __init__(self, own, full, ss, rs):
        self.own, self.full, self.ss, self.rs = own, full, ss, rs

    def start_z(self):
        z, x, c, _ = place()
        mine = blk(c, x, 16, z * 16)
        self.sent = []
        self.zc = [
            rcopy(self.own, self.full.at[mine], self.ss.at[d - 1], self.rs.at[d - 1], dev_z((z + d) % 8))
            for d in range(1, 8)
        ]
        self.full[mine, :] = self.own[...]

    def move(self, rows, k, dev):
        ref = self.full.at[rows]
        cp = rcopy(ref, ref, self.ss.at[k], self.rs.at[k], dev)
        self.sent.append(cp)
        return cp

    def start_x(self):
        z, x, c, _ = place()
        for cp in self.zc:
            cp.wait_recv()
        self.right = self.move(blk(c, x), 7, {"x": (x + 1) % 4})
        self.left = self.move(blk(c, x), 8, {"x": (x + 3) % 4})
        self.cores = [self.move(blk(c, x), 11, {"c": 1 - c})]

    def forward_x(self):
        z, x, c, _ = place()
        self.right.wait_recv()
        self.fr = self.move(blk(c, (x + 3) % 4, 64), 9, {"x": (x + 1) % 4})
        self.left.wait_recv()
        self.fl = self.move(blk(c, (x + 1) % 4, 64, 64), 10, {"x": (x + 3) % 4})
        self.cores.append(self.move(blk(c, (x + 3) % 4), 12, {"c": 1 - c}))
        self.cores.append(self.move(blk(c, (x + 1) % 4), 13, {"c": 1 - c}))

    def finish(self):
        z, x, c, _ = place()
        self.fr.wait_recv()
        self.fl.wait_recv()
        self.cores.append(self.move(blk(c, (x + 2) % 4), 14, {"c": 1 - c}))
        for cp in self.cores:
            cp.wait_recv()
        for cp in self.zc + self.sent:
            cp.wait_send()


def add_rows(dst, dst_at, terms, rows, step=32):
    for r in range(0, rows, step):
        total = None
        for ref, base in terms:
            v = ref[pl.ds(base + r, step), :].astype(F32)
            total = v if total is None else total + v
        dst[pl.ds(dst_at + r, step), :] = total.astype(dst.dtype)


class Reduce:
    sems = 4 + 2 + 4 + 7

    @staticmethod
    def scratch():
        return [
            pltpu.VMEM((512, 1024), BF),
            pltpu.VMEM((128, 1024), BF),
            pltpu.VMEM((128, 1024), BF),
            pltpu.VMEM((256, 1024), BF),
            pltpu.VMEM((256, 1024), BF),
            pltpu.VMEM((128, 1024), BF),
            pltpu.VMEM((112, 1024), BF),
        ]

    def __init__(self, part, bufs, ss, rs):
        self.part, self.ss, self.rs = part, ss, rs
        self.crecv, self.obuf, self.orecv, self.nbuf, self.xrecv, self.zbuf, self.zrecv = bufs
        self.sent = []

    def send(self, src, dst, k, dev):
        cp = rcopy(src, dst, self.ss.at[k], self.rs.at[k], dev)
        self.sent.append(cp)
        return cp

    def start_c(self):
        z, x, c, _ = place()
        self.cores = []
        for k, d in enumerate((2, 1, 3, 0)):
            xx = (x + d) % 4
            self.cores.append(
                self.send(
                    self.part.at[blk(1 - c, xx)],
                    self.crecv.at[pl.ds(pl.multiple_of(xx * 128, 128), 128)],
                    k,
                    {"c": 1 - c},
                )
            )

    def start_opposite(self):
        z, x, c, _ = place()
        self.cores[0].wait_recv()
        o = (x + 2) % 4
        terms = [(self.part, c * 512 + o * 128), (self.crecv, o * 128)]
        add_rows(self.obuf, 0, terms, 128)
        half = pl.ds(0, 64)
        rest = pl.ds(64, 64)
        self.o_right = self.send(self.obuf.at[half], self.orecv.at[half], 4, {"x": (x + 1) % 4})
        self.o_left = self.send(self.obuf.at[rest], self.orecv.at[rest], 5, {"x": (x + 3) % 4})

    def start_near(self):
        z, x, c, _ = place()
        r, l = (x + 1) % 4, (x + 3) % 4
        self.near = []
        self.cores[1].wait_recv()
        add_rows(self.nbuf, 64, [(self.part, c * 512 + r * 128 + 64), (self.crecv, r * 128 + 64)], 64)
        s = pl.ds(64, 64)
        self.near.append(self.send(self.nbuf.at[s], self.xrecv.at[s], 6, {"x": r}))
        self.cores[2].wait_recv()
        add_rows(self.nbuf, 128, [(self.part, c * 512 + l * 128), (self.crecv, l * 128)], 64)
        s = pl.ds(128, 64)
        self.near.append(self.send(self.nbuf.at[s], self.xrecv.at[s], 7, {"x": l}))

    def finish_near(self):
        z, x, c, _ = place()
        r, l = (x + 1) % 4, (x + 3) % 4
        self.o_right.wait_recv()
        add_rows(
            self.nbuf, 0,
            [(self.part, c * 512 + r * 128), (self.crecv, r * 128), (self.orecv, 0)], 64,
        )
        s = pl.ds(0, 64)
        self.near.append(self.send(self.nbuf.at[s], self.xrecv.at[s], 8, {"x": r}))
        self.o_left.wait_recv()
        add_rows(
            self.nbuf, 192,
            [(self.part, c * 512 + l * 128 + 64), (self.crecv, l * 128 + 64), (self.orecv, 64)], 64,
        )
        s = pl.ds(192, 64)
        self.near.append(self.send(self.nbuf.at[s], self.xrecv.at[s], 9, {"x": l}))

    def start_z(self):
        z, x, c, _ = place()
        self.cores[3].wait_recv()
        for cp in self.near:
            cp.wait_recv()
        terms = [(self.part, c * 512 + x * 128), (self.crecv, x * 128), (self.xrecv, 0), (self.xrecv, 128)]
        add_rows(self.zbuf, 0, terms, 128)
        self.zc = []
        for d in range(1, 8):
            t = (z + d) % 8
            src = self.zbuf.at[pl.ds(pl.multiple_of(t * 16, 16), 16)]
            self.zc.append(self.send(src, self.zrecv.at[pl.ds((d - 1) * 16, 16)], 9 + d, dev_z(t)))

    def total(self):
        z, x, c, _ = place()
        out = self.zbuf[pl.ds(pl.multiple_of(z * 16, 16), 16), :].astype(F32)
        for d in range(1, 8):
            self.zc[d - 1].wait_recv()
            out = out + self.zrecv[pl.ds((d - 1) * 16, 16), :].astype(F32)
        return out

    def drain(self):
        for cp in self.sent:
            cp.wait_send()


def opening_kernel(normed, cot, sbuf, normed_all, cot_all, w_in, w_out, rbuf, gs, gr, ws, wr, ys, yr):
    z, x, c, y = place()
    greet_all()
    exchange_start(sbuf, rbuf, ws, wr)
    a = Gather(normed, normed_all, gs.at[0], gr.at[0])
    b = Gather(cot, cot_all, gs.at[1], gr.at[1])
    a.start_z()
    b.start_z()
    exchange_wait(sbuf, rbuf, ws, wr)
    for h in range(2):
        def tile(q, _):
            v = [rbuf[h * 32 + q * 4 + i].astype(F32) for i in range(4)]
            rows = pl.ds(pl.multiple_of(q * 16, 16), 16)
            w_in[h, y, rows, :] = jnp.concatenate([u[0:4] for u in v], axis=0).astype(BF)
            w_out[h, y, rows, :] = jnp.concatenate([u[4:8] for u in v], axis=0).astype(BF)
            return 0

        lax.fori_loop(0, 8, tile, 0)
    up, down = {"y": (y + 1) % 4}, {"y": (y + 3) % 4}
    ups, downs = {}, {}
    for h in range(2):
        for m, w in enumerate((w_in, w_out)):
            k = h * 2 + m
            ups[h, m] = rcopy(w.at[h, y], w.at[h, y], ys.at[k], yr.at[k], up)
    for h in (1, 0):
        for m, w in enumerate((w_in, w_out)):
            k = 4 + h * 2 + m
            downs[h, m] = rcopy(w.at[h, y], w.at[h, y], ys.at[k], yr.at[k], down)
    a.start_x()
    b.start_x()
    a.forward_x()
    b.forward_x()
    far = []
    for m, w in enumerate((w_in, w_out)):
        ups[0, m].wait_recv()
        s = w.at[0, (y + 3) % 4]
        far.append(rcopy(s, s, ys.at[8 + m], yr.at[8 + m], up))
        downs[1, m].wait_recv()
        s = w.at[1, (y + 1) % 4]
        far.append(rcopy(s, s, ys.at[10 + m], yr.at[10 + m], down))
    a.finish()
    b.finish()
    for m in range(2):
        ups[1, m].wait_recv()
        downs[0, m].wait_recv()
    for cp in far:
        cp.wait_recv()
    for cp in far + list(ups.values()) + list(downs.values()):
        cp.wait_send()
    exchange_sent(sbuf, ws)


def opening(normed, cot, sbuf):
    tok = jax.ShapeDtypeStruct((1024, 1024), BF)
    wt = jax.ShapeDtypeStruct((2, 4, 128, 512), BF)
    n = Gather.sems
    dma = pltpu.SemaphoreType.DMA
    return pl.pallas_call(
        opening_kernel,
        name="opening",
        out_shape=(tok, tok, wt, wt),
        in_specs=[pl.BlockSpec(memory_space=pltpu.VMEM)] * 3,
        out_specs=(pl.BlockSpec(memory_space=pltpu.VMEM),) * 4,
        scratch_shapes=[
            pltpu.VMEM((64, 8, 512), BF),
            dma((2, n)), dma((2, n)), dma, dma, dma((12,)), dma((12,)),
        ],
        compiler_params=pltpu.CompilerParams(collective_id=0, has_side_effects=True, vmem_limit_bytes=40 * 2**20),
        cost_estimate=pl.CostEstimate(flops=40_000_000_000, bytes_accessed=2**23, transcendentals=0),
    )(normed, cot, sbuf)


def turn_kernel(first, part, base, gain, aux, new, full, *scratch):
    n = len(Reduce.scratch())
    bufs, (own, gs, gr, rs, rr) = scratch[:n], scratch[n:]
    greet(peers_near(False))
    r = Reduce(part, bufs, rs, rr)
    r.start_c()
    r.start_opposite()
    r.start_near()
    r.finish_near()
    r.start_z()
    total = r.total()
    if first:
        new_val = (base[...].astype(F32) + total).astype(BF)
        f = new_val.astype(F32)
        inv = lax.rsqrt(jnp.mean(f * f, axis=1, keepdims=True) + norm_eps)
        own[...] = (f * inv * gain[...]).astype(BF)
        new[...] = new_val
        src = own
    else:
        f = aux[...].astype(F32)
        inv = lax.rsqrt(jnp.mean(f * f, axis=1, keepdims=True) + norm_eps)
        gated = total * gain[...]
        new[...] = (
            base[...].astype(F32)
            + inv * gated
            - f * inv * inv * inv * jnp.mean(f * gated, axis=1, keepdims=True)
        ).astype(BF)
        src = new
    g = Gather(src, full, gs, gr)
    g.start_z()
    r.drain()
    g.start_x()
    g.forward_x()
    g.finish()


def turn(first, part, base, gain, aux):
    dma = pltpu.SemaphoreType.DMA
    return pl.pallas_call(
        functools.partial(turn_kernel, first),
        name="turn_one" if first else "turn_two",
        out_shape=(jax.ShapeDtypeStruct((16, 1024), BF), jax.ShapeDtypeStruct((1024, 1024), BF)),
        in_specs=[pl.BlockSpec(memory_space=pltpu.VMEM)] * 4,
        out_specs=(pl.BlockSpec(memory_space=pltpu.VMEM),) * 2,
        scratch_shapes=Reduce.scratch()
        + [pltpu.VMEM((16, 1024), BF), dma((Gather.sems,)), dma((Gather.sems,)), dma((Reduce.sems,)), dma((Reduce.sems,))],
        compiler_params=pltpu.CompilerParams(collective_id=1 if first else 2, has_side_effects=True, vmem_limit_bytes=40 * 2**20),
        cost_estimate=pl.CostEstimate(flops=40_000_000_000, bytes_accessed=2**23, transcendentals=0),
    )(part, base, gain, aux)


def closing_kernel(part_a, part_b, g_in, g_out, sum_a, sum_b, rbuf, *scratch):
    n = len(Reduce.scratch())
    bufs_a, bufs_b = scratch[:n], scratch[n : 2 * n]
    oh, orv, nh, xr_in, sbuf, rs, rr, ys, yr, ws, wr = scratch[2 * n :]
    z, x, c, y = place()
    greet_all()
    up, down = {"y": (y + 1) % 4}, {"y": (y + 3) % 4}
    u, d, o = (y + 1) % 4, (y + 3) % 4, (y + 2) % 4
    gr = (g_in, g_out)
    sent, opp, plain, mixed = [], [], [], []
    for m in range(2):
        opp.append(rcopy(gr[m].at[0, o], orv.at[m, 0], ys.at[m], yr.at[m], up))
        opp.append(rcopy(gr[m].at[1, o], orv.at[m, 1], ys.at[2 + m], yr.at[2 + m], down))
    for m in range(2):
        plain.append(rcopy(gr[m].at[1, u], xr_in.at[m, 0, 1], ys.at[4 + m], yr.at[4 + m], up))
        plain.append(rcopy(gr[m].at[0, d], xr_in.at[m, 1, 0], ys.at[6 + m], yr.at[6 + m], down))
    a = Reduce(part_b, bufs_b, rs.at[0], rr.at[0])
    b = Reduce(part_a, bufs_a, rs.at[1], rr.at[1])
    for r in (a, b):
        r.start_c()
    for r in (a, b):
        r.start_opposite()
    for r in (a, b):
        r.start_near()
    for m in range(2):
        opp[2 * m].wait_recv()
        for s in range(0, 128, 32):
            nh[m, 0, s : s + 32, :] = (
                gr[m][0, u, s : s + 32, :].astype(F32) + orv[m, 0, s : s + 32, :].astype(F32)
            ).astype(BF)
        mixed.append(rcopy(nh.at[m, 0], xr_in.at[m, 0, 0], ys.at[8 + m], yr.at[8 + m], up))
        opp[2 * m + 1].wait_recv()
        for s in range(0, 128, 32):
            nh[m, 1, s : s + 32, :] = (
                gr[m][1, d, s : s + 32, :].astype(F32) + orv[m, 1, s : s + 32, :].astype(F32)
            ).astype(BF)
        mixed.append(rcopy(nh.at[m, 1], xr_in.at[m, 1, 1], ys.at[10 + m], yr.at[10 + m], down))
    for r in (a, b):
        r.finish_near()
    for r in (a, b):
        r.start_z()
    for cp in plain + mixed:
        cp.wait_recv()
    for h in range(2):
        def tile(q, _):
            rows = pl.ds(pl.multiple_of(q * 16, 16), 16)
            t = [
                gr[m][h, y, rows, :].astype(F32)
                + xr_in[m, 0, h, rows, :].astype(F32)
                + xr_in[m, 1, h, rows, :].astype(F32)
                for m in range(2)
            ]
            for i in range(4):
                sbuf[h * 32 + q * 4 + i] = jnp.concatenate(
                    [t[0][4 * i : 4 * i + 4], t[1][4 * i : 4 * i + 4]], axis=0
                ).astype(BF)
            return 0

        lax.fori_loop(0, 8, tile, 0)
    exchange_start(sbuf, rbuf, ws, wr)
    sum_b[...] = a.total()
    sum_a[...] = b.total()
    exchange_wait(sbuf, rbuf, ws, wr)
    exchange_sent(sbuf, ws)
    a.drain()
    b.drain()
    for cp in opp + plain + mixed:
        cp.wait_send()


def closing(part_a, part_b, g_in, g_out):
    dma = pltpu.SemaphoreType.DMA
    tok = jax.ShapeDtypeStruct((16, 1024), F32)
    return pl.pallas_call(
        closing_kernel,
        name="closing",
        out_shape=(tok, tok, jax.ShapeDtypeStruct((64, 8, 512), BF)),
        in_specs=[pl.BlockSpec(memory_space=pltpu.VMEM)] * 4,
        out_specs=(pl.BlockSpec(memory_space=pltpu.VMEM),) * 3,
        scratch_shapes=Reduce.scratch() * 2
        + [
            pltpu.VMEM((2, 2, 128, 512), BF),
            pltpu.VMEM((2, 2, 128, 512), BF),
            pltpu.VMEM((2, 2, 128, 512), BF),
            pltpu.VMEM((2, 2, 2, 128, 512), BF),
            pltpu.VMEM((64, 8, 512), BF),
            dma((2, Reduce.sems)), dma((2, Reduce.sems)), dma((12,)), dma((12,)), dma, dma,
        ],
        compiler_params=pltpu.CompilerParams(collective_id=3, has_side_effects=True, vmem_limit_bytes=48 * 2**20),
        cost_estimate=pl.CostEstimate(flops=40_000_000_000, bytes_accessed=2**23, transcendentals=0),
    )(part_a, part_b, g_in, g_out)


def pick_kernel(idx, slots, w_in, w_out):
    for k in range(16):
        w_in[k * 64 : (k + 1) * 64, :] = slots[idx[0, k], 0:64, :]
        w_out[k * 64 : (k + 1) * 64, :] = slots[idx[1, k], 64:128, :]


def pick(idx, slots):
    wt = jax.ShapeDtypeStruct((1024, 512), BF)
    return pl.pallas_call(
        pick_kernel,
        name="pick",
        out_shape=(wt, wt),
        in_specs=[pl.BlockSpec(memory_space=pltpu.SMEM), pl.BlockSpec(memory_space=pltpu.VMEM)],
        out_specs=(pl.BlockSpec(memory_space=pltpu.VMEM),) * 2,
        cost_estimate=pl.CostEstimate(flops=4_000_000_000, bytes_accessed=2**22, transcendentals=0),
    )(idx, slots)


def place_kernel(idx, live, g_in, g_out, slots):
    for k in range(24):
        for m, g in enumerate((g_in, g_out)):
            v = g[idx[m, k]]
            keep = jnp.full(v.shape, live[m, k], jnp.int32) > 0
            slots[k, m * 64 : (m + 1) * 64, :] = jnp.where(keep, v.astype(F32), 0.0).astype(BF)


def place_slots(idx, live, g_in, g_out):
    return pl.pallas_call(
        place_kernel,
        name="place",
        out_shape=jax.ShapeDtypeStruct((24, 128, 512), BF),
        in_specs=[pl.BlockSpec(memory_space=pltpu.SMEM)] * 2 + [pl.BlockSpec(memory_space=pltpu.VMEM)] * 2,
        out_specs=pl.BlockSpec(memory_space=pltpu.VMEM),
        cost_estimate=pl.CostEstimate(flops=4_000_000_000, bytes_accessed=2**22, transcendentals=0),
    )(idx, live, g_in.reshape(16, 64, 512), g_out.reshape(16, 64, 512))


def dot(a, b, dims, kind=F32):
    return lax.dot_general(a, b, (dims, ((), ())), preferred_element_type=F32).astype(kind)


def shards(
    tokens, grad_out, gains, flat_in, flat_out, flat_moment, flat_second,
    tile_in, tile_out, tile_moment, tile_second, owners,
):
    zh, y = at("zh"), at("y")
    row = zh * 4 + y
    swap = [(0, 1), (1, 0)]

    slot_dest, slot_tile, slot_live = slot_tables(owners[:, 0, :], 3, 8)
    both = jnp.concatenate([tile_in[0], tile_out[0]], axis=1)
    lo, hi = both[:, :, :512], both[:, :, 512:]
    keep, give = jnp.where(zh == 0, lo, hi), jnp.where(zh == 0, hi, lo)
    taken = lax.ppermute(give, "zh", swap)
    slots = lax.all_gather(jnp.concatenate([keep, taken], axis=0), "y", axis=0, tiled=True)
    dest_row, dest_slot = slot_dest // 3, slot_dest % 3
    dest_at = (dest_row % 4) * 6 + ((dest_row // 4) ^ zh) * 3 + dest_slot
    p = jnp.arange(24)
    p_slot = (((p // 3) % 2 ^ zh) * 4 + p // 6) * 3 + p % 3
    out_tile = jnp.take(slot_tile, p_slot, axis=1)
    out_live = jnp.take(slot_live.astype(jnp.int32), p_slot, axis=1)

    tok_float = tokens.astype(F32)
    inv_one = lax.rsqrt(jnp.mean(tok_float * tok_float, axis=1, keepdims=True) + norm_eps)
    normed = (tok_float * inv_one * gains[0]).astype(BF)
    flat = jnp.stack([flat_in.reshape(4, 32, 2, 512), flat_out.reshape(4, 32, 2, 512)])
    sbuf = flat.transpose(3, 2, 0, 1, 4).reshape(64, 8, 512)
    normed_one, cot_two, w_in_one, w_out_one = opening(normed, grad_out, sbuf)
    w_in_one, w_out_one = w_in_one.reshape(1024, 512), w_out_one.reshape(1024, 512)

    hidden_one = dot(normed_one, w_in_one, ((1,), (0,)))
    act_one = gelu_value(hidden_one).astype(BF)
    part = dot(act_one, w_out_one, ((1,), (1,)), BF)
    middle, normed_two = turn(True, part, tokens, gains[1:2], tokens)

    w_in_two, w_out_two = pick(dest_at, slots)
    hidden_two = dot(normed_two, w_in_two, ((1,), (0,)))
    act_two = gelu_value(hidden_two).astype(BF)
    d_act_two = dot(cot_two, w_out_two, ((1,), (0,)))
    d_hidden_two = (d_act_two * gelu_slope(hidden_two)).astype(BF)
    part = dot(d_hidden_two, w_in_two, ((1,), (1,)), BF)
    grad_in_two = dot(normed_two, d_hidden_two, ((0,), (0,)), BF)
    grad_out_two = dot(cot_two, act_two, ((0,), (0,)), BF)
    outgoing = place_slots(out_tile, out_live, grad_in_two, grad_out_two)
    summed = lax.psum_scatter(outgoing, "y", scatter_dimension=0, tiled=True)
    part_two = dot(act_two, w_out_two, ((1,), (1,)), BF)
    grad_mid, cot_one = turn(False, part, grad_out, gains[1:2], middle)

    d_act_one = dot(cot_one, w_out_one, ((1,), (0,)))
    d_hidden_one = (d_act_one * gelu_slope(hidden_one)).astype(BF)
    part = dot(d_hidden_one, w_in_one, ((1,), (1,)), BF)
    grad_in_one = dot(normed_one, d_hidden_one, ((0,), (0,)), BF).reshape(2, 4, 128, 512)
    grad_out_one = dot(cot_one, act_one, ((0,), (0,)), BF).reshape(2, 4, 128, 512)
    sum_two, d_normed, rbuf = closing(part_two, part, grad_in_one, grad_out_one)

    hidden_out = (middle.astype(F32) + sum_two).astype(BF)
    gated = d_normed * gains[0]
    grad_tokens = (
        grad_mid.astype(F32)
        + inv_one * gated
        - tok_float * inv_one * inv_one * inv_one * jnp.mean(tok_float * gated, axis=1, keepdims=True)
    ).astype(BF)

    flat_grad = rbuf.reshape(2, 32, 2, 4, 512).transpose(2, 3, 1, 0, 4).reshape(2, 128, 1024).astype(F32)
    new_flat_in, m_in, v_in = adam_update(flat_in, flat_grad[0], flat_moment[0], flat_second[0])
    new_flat_out, m_out, v_out = adam_update(flat_out, flat_grad[1], flat_moment[1], flat_second[1])

    mine, other = summed[:3], lax.ppermute(summed[3:], "zh", swap)
    lo, hi = jnp.where(zh == 0, mine, other), jnp.where(zh == 0, other, mine)
    tile_grad = jnp.concatenate([lo, hi], axis=2).astype(F32)
    live = lax.dynamic_slice_in_dim(slot_live, row * 3, 3, 1)
    new_tiles, tms, tss = [], [], []
    for m, w in enumerate((tile_in[0], tile_out[0])):
        mask = live[m][:, None, None]
        g = tile_grad[:, m * 64 : (m + 1) * 64, :]
        w2, m2, v2 = adam_update(w, g, tile_moment[m, 0], tile_second[m, 0])
        new_tiles.append(jnp.where(mask, w2, w)[None])
        tms.append(jnp.where(mask, m2, tile_moment[m, 0]))
        tss.append(jnp.where(mask, v2, tile_second[m, 0]))
    return (
        hidden_out, grad_tokens, new_flat_in, new_flat_out,
        jnp.stack([m_in, m_out]), jnp.stack([v_in, v_out]),
        new_tiles[0], new_tiles[1], jnp.stack(tms)[:, None], jnp.stack(tss)[:, None],
    )


def solution(mesh):
    mesh = Mesh(mesh.devices.reshape(2, 4, 4, 4, 2), ALL)
    whole = P(ALL, None)
    state = P(None, ALL, None)
    tile = P(COL, ROW, None, None)
    tile_state = P(None, COL, ROW, None, None)
    return jax.shard_map(
        shards,
        mesh=mesh,
        in_specs=(whole, whole, P(), whole, whole, state, state, tile, tile, tile_state, tile_state, P(None, COL, None)),
        out_specs=(whole, whole, whole, whole, state, state, tile, tile, tile_state, tile_state),
        check_vma=False,
    )
```

```python
import functools

import jax
import jax.numpy as jnp
from jax import lax
from jax.experimental import pallas as pl
from jax.experimental.pallas import tpu as pltpu
from jax.sharding import Mesh, PartitionSpec as P

norm_eps = 1e-06
beta_one = 0.9
beta_two = 0.95
learn_rate = 0.002
decay_rate = 0.1
adam_eps = 1e-08
gelu_coef = 0.7978845608

ALL = ("zh", "y", "zl", "x", "c")
ROW = ("zh", "y")
COL = ("zl", "x", "c")
MESH = pl.DeviceIdType.MESH
BF = jnp.bfloat16
F32 = jnp.float32

def gelu_value(hidden):
    tanh_term = jnp.tanh(gelu_coef * (hidden + 0.044715 * hidden * hidden * hidden))
    return 0.5 * hidden * (1.0 + tanh_term)


def gelu_slope(hidden):
    tanh_term = jnp.tanh(gelu_coef * (hidden + 0.044715 * hidden * hidden * hidden))
    return 0.5 * (1.0 + tanh_term) + 0.5 * hidden * (1.0 - tanh_term * tanh_term) * gelu_coef * (
        1.0 + 0.134145 * hidden * hidden
    )


def adam_update(weight, gradient, moment, second):
    new_moment = beta_one * moment + (1.0 - beta_one) * gradient
    new_second = beta_two * second + (1.0 - beta_two) * gradient * gradient
    weight_float = weight.astype(jnp.float32)
    stepped = weight_float - learn_rate * (
        new_moment / (jnp.sqrt(new_second) + adam_eps) + decay_rate * weight_float
    )
    return (stepped.astype(jnp.bfloat16), new_moment, new_second)


def dev_z(z):
    return {"zh": z // 4, "zl": z % 4}


def at(a):
    return lax.axis_index(a)


def place():
    return at("zh") * 4 + at("zl"), at("x"), at("c"), at("y")


def peers_near(with_y):
    z, x, c, y = place()
    peers = [dev_z((z + d) % 8) for d in range(1, 8)]
    peers += [{"x": (x + 1) % 4}, {"x": (x + 3) % 4}, {"c": 1 - c}]
    if with_y:
        peers += [{"y": (y + 1) % 4}, {"y": (y + 3) % 4}]
    return peers


def greet(peers):
    sem = pltpu.get_barrier_semaphore()
    for p in peers:
        pl.semaphore_signal(sem, inc=1, device_id=p, device_id_type=MESH)
    pl.semaphore_wait(sem, len(peers))


def flat_dev(t):
    return {"zh": t // 32, "zl": (t // 8) % 4, "x": (t // 2) % 4, "c": t % 2}


def my_flat():
    z, x, c, _ = place()
    return z * 8 + x * 2 + c


def greet_all():
    me = my_flat()
    y = at("y")
    sem = pltpu.get_barrier_semaphore()

    def one(o, _):
        pl.semaphore_signal(sem, inc=1, device_id=flat_dev((me + o) % 64), device_id_type=MESH)
        return 0

    lax.fori_loop(1, 64, one, 0)
    for d in (1, 3):
        pl.semaphore_signal(sem, inc=1, device_id={"y": (y + d) % 4}, device_id_type=MESH)
    pl.semaphore_wait(sem, 65)


def rcopy(src, dst, ssem, rsem, dev):
    cp = pltpu.make_async_remote_copy(
        src_ref=src, dst_ref=dst, send_sem=ssem, recv_sem=rsem, device_id=dev, device_id_type=MESH
    )
    cp.start()
    return cp


def exchange_start(sbuf, rbuf, ssem, rsem):
    me = my_flat()

    def one(o, _):
        t = (me + o) % 64
        rcopy(sbuf.at[t], rbuf.at[me], ssem, rsem, flat_dev(t))
        return 0

    lax.fori_loop(1, 64, one, 0)
    rbuf[me] = sbuf[me]


def exchange_wait(sbuf, rbuf, ssem, rsem):
    part = pltpu.make_async_copy(rbuf.at[pl.ds(0, 63)], rbuf.at[pl.ds(0, 63)], rsem)
    part.wait()


def exchange_sent(sbuf, ssem):
    part = pltpu.make_async_copy(sbuf.at[pl.ds(0, 63)], sbuf.at[pl.ds(0, 63)], ssem)
    part.wait()


def blk(c, x, n=128, off=0):
    return pl.ds(pl.multiple_of(c * 512 + x * 128 + off, 16), n)


class Gather:
    sems = 7 + 2 + 2 + 4

    def __init__(self, own, full, ss, rs):
        self.own, self.full, self.ss, self.rs = own, full, ss, rs

    def start_z(self):
        z, x, c, _ = place()
        mine = blk(c, x, 16, z * 16)
        self.sent = []
        self.zc = [
            rcopy(self.own, self.full.at[mine], self.ss.at[d - 1], self.rs.at[d - 1], dev_z((z + d) % 8))
            for d in range(1, 8)
        ]
        self.full[mine, :] = self.own[...]

    def move(self, rows, k, dev):
        ref = self.full.at[rows]
        cp = rcopy(ref, ref, self.ss.at[k], self.rs.at[k], dev)
        self.sent.append(cp)
        return cp

    def start_x(self):
        z, x, c, _ = place()
        for cp in self.zc:
            cp.wait_recv()
        self.right = self.move(blk(c, x), 7, {"x": (x + 1) % 4})
        self.left = self.move(blk(c, x), 8, {"x": (x + 3) % 4})
        self.cores = [self.move(blk(c, x), 11, {"c": 1 - c})]

    def forward_x(self):
        z, x, c, _ = place()
        self.right.wait_recv()
        self.fr = self.move(blk(c, (x + 3) % 4, 64), 9, {"x": (x + 1) % 4})
        self.left.wait_recv()
        self.fl = self.move(blk(c, (x + 1) % 4, 64, 64), 10, {"x": (x + 3) % 4})
        self.cores.append(self.move(blk(c, (x + 3) % 4), 12, {"c": 1 - c}))
        self.cores.append(self.move(blk(c, (x + 1) % 4), 13, {"c": 1 - c}))

    def finish(self):
        z, x, c, _ = place()
        self.fr.wait_recv()
        self.fl.wait_recv()
        self.cores.append(self.move(blk(c, (x + 2) % 4), 14, {"c": 1 - c}))
        for cp in self.cores:
            cp.wait_recv()
        for cp in self.zc + self.sent:
            cp.wait_send()


def add_rows(dst, dst_at, terms, rows, step=32):
    for r in range(0, rows, step):
        total = None
        for ref, base in terms:
            v = ref[pl.ds(base + r, step), :].astype(F32)
            total = v if total is None else total + v
        dst[pl.ds(dst_at + r, step), :] = total.astype(dst.dtype)


class Reduce:
    sems = 4 + 2 + 4 + 7

    @staticmethod
    def scratch():
        return [
            pltpu.VMEM((512, 1024), BF),
            pltpu.VMEM((128, 1024), BF),
            pltpu.VMEM((128, 1024), BF),
            pltpu.VMEM((256, 1024), BF),
            pltpu.VMEM((256, 1024), BF),
            pltpu.VMEM((128, 1024), BF),
            pltpu.VMEM((112, 1024), BF),
        ]

    def __init__(self, part, bufs, ss, rs):
        self.part, self.ss, self.rs = part, ss, rs
        self.crecv, self.obuf, self.orecv, self.nbuf, self.xrecv, self.zbuf, self.zrecv = bufs
        self.sent = []

    def send(self, src, dst, k, dev):
        cp = rcopy(src, dst, self.ss.at[k], self.rs.at[k], dev)
        self.sent.append(cp)
        return cp

    def start_c(self):
        z, x, c, _ = place()
        self.cores = []
        for k, d in enumerate((2, 1, 3, 0)):
            xx = (x + d) % 4
            self.cores.append(
                self.send(
                    self.part.at[blk(1 - c, xx)],
                    self.crecv.at[pl.ds(pl.multiple_of(xx * 128, 128), 128)],
                    k,
                    {"c": 1 - c},
                )
            )

    def start_opposite(self):
        z, x, c, _ = place()
        self.cores[0].wait_recv()
        o = (x + 2) % 4
        terms = [(self.part, c * 512 + o * 128), (self.crecv, o * 128)]
        add_rows(self.obuf, 0, terms, 128)
        half = pl.ds(0, 64)
        rest = pl.ds(64, 64)
        self.o_right = self.send(self.obuf.at[half], self.orecv.at[half], 4, {"x": (x + 1) % 4})
        self.o_left = self.send(self.obuf.at[rest], self.orecv.at[rest], 5, {"x": (x + 3) % 4})

    def start_near(self):
        z, x, c, _ = place()
        r, l = (x + 1) % 4, (x + 3) % 4
        self.near = []
        self.cores[1].wait_recv()
        add_rows(self.nbuf, 64, [(self.part, c * 512 + r * 128 + 64), (self.crecv, r * 128 + 64)], 64)
        s = pl.ds(64, 64)
        self.near.append(self.send(self.nbuf.at[s], self.xrecv.at[s], 6, {"x": r}))
        self.cores[2].wait_recv()
        add_rows(self.nbuf, 128, [(self.part, c * 512 + l * 128), (self.crecv, l * 128)], 64)
        s = pl.ds(128, 64)
        self.near.append(self.send(self.nbuf.at[s], self.xrecv.at[s], 7, {"x": l}))

    def finish_near(self):
        z, x, c, _ = place()
        r, l = (x + 1) % 4, (x + 3) % 4
        self.o_right.wait_recv()
        add_rows(
            self.nbuf, 0,
            [(self.part, c * 512 + r * 128), (self.crecv, r * 128), (self.orecv, 0)], 64,
        )
        s = pl.ds(0, 64)
        self.near.append(self.send(self.nbuf.at[s], self.xrecv.at[s], 8, {"x": r}))
        self.o_left.wait_recv()
        add_rows(
            self.nbuf, 192,
            [(self.part, c * 512 + l * 128 + 64), (self.crecv, l * 128 + 64), (self.orecv, 64)], 64,
        )
        s = pl.ds(192, 64)
        self.near.append(self.send(self.nbuf.at[s], self.xrecv.at[s], 9, {"x": l}))

    def start_z(self):
        z, x, c, _ = place()
        self.cores[3].wait_recv()
        for cp in self.near:
            cp.wait_recv()
        terms = [(self.part, c * 512 + x * 128), (self.crecv, x * 128), (self.xrecv, 0), (self.xrecv, 128)]
        add_rows(self.zbuf, 0, terms, 128)
        self.zc = []
        for d in range(1, 8):
            t = (z + d) % 8
            src = self.zbuf.at[pl.ds(pl.multiple_of(t * 16, 16), 16)]
            self.zc.append(self.send(src, self.zrecv.at[pl.ds((d - 1) * 16, 16)], 9 + d, dev_z(t)))

    def total(self):
        z, x, c, _ = place()
        out = self.zbuf[pl.ds(pl.multiple_of(z * 16, 16), 16), :].astype(F32)
        for d in range(1, 8):
            self.zc[d - 1].wait_recv()
            out = out + self.zrecv[pl.ds((d - 1) * 16, 16), :].astype(F32)
        return out

    def drain(self):
        for cp in self.sent:
            cp.wait_send()


class YGather:
    def __init__(self, own, full, ss, rs):
        self.own, self.full, self.ss, self.rs = own, full, ss, rs

    def copy(self, src, m, h, yy, k, dev):
        return rcopy(src, self.full[m].at[h, yy], self.ss.at[k], self.rs.at[k], dev)

    def start(self):
        y = at("y")
        self.up, self.down = {"y": (y + 1) % 4}, {"y": (y + 3) % 4}
        self.ups, self.downs = {}, {}
        for h in range(2):
            for m in range(2):
                self.ups[h, m] = self.copy(self.own(m, h), m, h, y, h * 2 + m, self.up)
        for h in (1, 0):
            for m in range(2):
                self.downs[h, m] = self.copy(self.own(m, h), m, h, y, 4 + h * 2 + m, self.down)

    def forward(self):
        y = at("y")
        self.far = []
        for m in range(2):
            self.ups[0, m].wait_recv()
            yy = (y + 3) % 4
            self.far.append(self.copy(self.full[m].at[0, yy], m, 0, yy, 8 + m, self.up))
            self.downs[1, m].wait_recv()
            yy = (y + 1) % 4
            self.far.append(self.copy(self.full[m].at[1, yy], m, 1, yy, 10 + m, self.down))

    def finish(self):
        for m in range(2):
            self.ups[1, m].wait_recv()
            self.downs[0, m].wait_recv()
        for cp in self.far:
            cp.wait_recv()

    def drain(self):
        for cp in self.far + list(self.ups.values()) + list(self.downs.values()):
            cp.wait_send()


class YReduce:
    @staticmethod
    def scratch(rows):
        return [
            pltpu.VMEM((2, 2, rows, 512), BF),
            pltpu.VMEM((2, 2, rows, 512), BF),
            pltpu.VMEM((2, 2, 2, rows, 512), BF),
        ]

    def __init__(self, part, rows, bufs, ss, rs):
        self.part, self.rows, self.ss, self.rs = part, rows, ss, rs
        self.orv, self.nh, self.xin = bufs

    def copy(self, src, dst, k, dev):
        return rcopy(src, dst, self.ss.at[k], self.rs.at[k], dev)

    def start(self):
        y = at("y")
        self.up, self.down = {"y": (y + 1) % 4}, {"y": (y + 3) % 4}
        u, d, o = (y + 1) % 4, (y + 3) % 4, (y + 2) % 4
        self.opp, self.plain, self.mixed = [], [], []
        for m in range(2):
            self.opp.append(self.copy(self.part[m].at[0, o], self.orv.at[m, 0], m, self.up))
            self.opp.append(self.copy(self.part[m].at[1, o], self.orv.at[m, 1], 2 + m, self.down))
        for m in range(2):
            self.plain.append(self.copy(self.part[m].at[1, u], self.xin.at[m, 0, 1], 4 + m, self.up))
            self.plain.append(self.copy(self.part[m].at[0, d], self.xin.at[m, 1, 0], 6 + m, self.down))

    def middle(self):
        y = at("y")
        u, d = (y + 1) % 4, (y + 3) % 4
        for m in range(2):
            for h, yy, dev in ((0, u, self.up), (1, d, self.down)):
                self.opp[2 * m + h].wait_recv()
                for s in range(0, self.rows, 32):
                    self.nh[m, h, s : s + 32, :] = (
                        self.part[m][h, yy, s : s + 32, :].astype(F32) + self.orv[m, h, s : s + 32, :].astype(F32)
                    ).astype(BF)
                self.mixed.append(self.copy(self.nh.at[m, h], self.xin.at[m, h, h], 8 + 2 * h + m, dev))

    def finish(self):
        for cp in self.plain + self.mixed:
            cp.wait_recv()

    def total(self, m, h, rows):
        return (
            self.part[m][h, at("y"), rows, :].astype(F32)
            + self.xin[m, 0, h, rows, :].astype(F32)
            + self.xin[m, 1, h, rows, :].astype(F32)
        )

    def drain(self):
        for cp in self.opp + self.plain + self.mixed:
            cp.wait_send()


def inv_rms(f):
    return lax.rsqrt(jnp.mean(f * f, axis=1, keepdims=True) + norm_eps)


def slot_of(owners, m, k):
    own, rank = owners[m, k], jnp.int32(0)
    for j in range(16):
        rank = rank + jnp.where((owners[m, j] == own) & (j < k), 1, 0)
    return own * 3 + rank


def ones_if(hit):
    return jnp.full((64, 512), jnp.where(hit, 1.0, 0.0), F32).astype(BF)


def half(h):
    return pl.ds(pl.multiple_of(h * 512, 128), 512)


def opening_kernel(
    tokens, cot, gains, sbuf, t_in, t_out, normed_all, cot_all, w_in, w_out, pair, rbuf, normed, gs, gr, ws, wr, ys, yr, ps, pr
):
    z, x, c, y = place()
    zh = at("zh")
    f = tokens[...].astype(F32)
    normed[...] = (f * inv_rms(f) * gains[0:1, :]).astype(BF)
    greet_all()
    exchange_start(sbuf, rbuf, ws, wr)
    a = Gather(normed, normed_all, gs.at[0], gr.at[0])
    b = Gather(cot, cot_all, gs.at[1], gr.at[1])
    a.start_z()
    b.start_z()
    pairs = [
        rcopy(t.at[:, :, half(1 - zh)], pair.at[m, zh], ps.at[m], pr.at[m], {"zh": 1 - zh})
        for m, t in enumerate((t_in, t_out))
    ]
    for m, t in enumerate((t_in, t_out)):
        pair[m, zh] = t[:, :, half(zh)]
    exchange_wait(sbuf, rbuf, ws, wr)
    for h in range(2):
        def tile(q, _):
            v = [rbuf[h * 32 + q * 4 + i].astype(F32) for i in range(4)]
            rows = pl.ds(pl.multiple_of(q * 16, 16), 16)
            w_in[h, y, rows, :] = jnp.concatenate([u[0:4] for u in v], axis=0).astype(BF)
            w_out[h, y, rows, :] = jnp.concatenate([u[4:8] for u in v], axis=0).astype(BF)
            return 0

        lax.fori_loop(0, 8, tile, 0)
    full = (w_in, w_out)
    yg = YGather(lambda m, h: full[m].at[h, y], full, ys, yr)
    yg.start()
    a.start_x()
    b.start_x()
    a.forward_x()
    yg.forward()
    b.forward_x()
    a.finish()
    b.finish()
    yg.finish()
    for cp in pairs:
        cp.wait_recv()
        cp.wait_send()
    yg.drain()
    exchange_sent(sbuf, ws)


VM = pl.BlockSpec(memory_space=pltpu.VMEM)
SM = pl.BlockSpec(memory_space=pltpu.SMEM)
DMA = pltpu.SemaphoreType.DMA


def comm_call(kernel, name, ident, out_shape, scratch, in_specs, args):
    return pl.pallas_call(
        kernel,
        name=name,
        out_shape=out_shape,
        in_specs=in_specs,
        out_specs=(VM,) * len(out_shape),
        scratch_shapes=scratch,
        compiler_params=pltpu.CompilerParams(collective_id=ident, has_side_effects=True, vmem_limit_bytes=56 * 2**20),
        cost_estimate=pl.CostEstimate(flops=40_000_000_000, bytes_accessed=2**23, transcendentals=0),
    )(*args)


def shape(*dims, kind=BF):
    return jax.ShapeDtypeStruct(dims, kind)


def opening(*args):
    n = Gather.sems
    out = (shape(1024, 1024), shape(1024, 1024), shape(2, 4, 128, 512), shape(2, 4, 128, 512), shape(2, 2, 3, 64, 512))
    scratch = [
        pltpu.VMEM((64, 8, 512), BF), pltpu.VMEM((16, 1024), BF),
        DMA((2, n)), DMA((2, n)), DMA, DMA, DMA((12,)), DMA((12,)), DMA((2,)), DMA((2,)),
    ]
    return comm_call(opening_kernel, "opening", 0, out, scratch, [VM] * 6, args)


def turn_one_kernel(owners, part, tokens, gains, pair, new, full, w_in, w_out, s_in, s_out, *scratch):
    n = len(Reduce.scratch())
    bufs, (own, gs, gr, rs, rr, ys, yr) = scratch[:n], scratch[n:]
    y = at("y")
    slots = (s_in, s_out)
    greet(peers_near(True))
    r = Reduce(part, bufs, rs, rr)
    r.start_c()
    yg = YGather(lambda m, h: pair.at[m, h], slots, ys, yr)
    yg.start()
    r.start_opposite()
    r.start_near()
    for m in range(2):
        for h in range(2):
            slots[m][h, y] = pair[m, h]
    r.finish_near()
    yg.forward()
    r.start_z()
    total = r.total()
    mid = (tokens[...].astype(F32) + total).astype(BF)
    f = mid.astype(F32)
    own[...] = (f * inv_rms(f) * gains[1:2, :]).astype(BF)
    new[...] = mid
    g = Gather(own, full, gs, gr)
    g.start_z()
    r.drain()
    g.start_x()
    yg.finish()
    for m, w in enumerate((w_in, w_out)):
        def tile(k, _, m=m, w=w):
            want = slot_of(owners, m, k)
            total = jnp.zeros((64, 512), BF)
            for q in range(24):
                r, s = q // 3, q % 3
                total = total + slots[m][r // 4, r % 4, s * 64 : (s + 1) * 64, :] * ones_if(want == q)
            w[pl.ds(pl.multiple_of(k * 64, 64), 64), :] = total
            return 0

        lax.fori_loop(0, 16, tile, 0)
    g.forward_x()
    g.finish()
    yg.drain()


def turn_one(*args):
    out = (shape(16, 1024), shape(1024, 1024), shape(1024, 512), shape(1024, 512))
    scratch = [pltpu.VMEM((2, 4, 192, 512), BF)] * 2 + Reduce.scratch() + [
        pltpu.VMEM((16, 1024), BF), DMA((Gather.sems,)), DMA((Gather.sems,)), DMA((Reduce.sems,)), DMA((Reduce.sems,)),
        DMA((12,)), DMA((12,)),
    ]
    return comm_call(turn_one_kernel, "turn_one", 1, out, scratch, [SM] + [VM] * 4, args)


def before_input(f, inv, gated, base):
    return base + inv * gated - f * inv * inv * inv * jnp.mean(f * gated, axis=1, keepdims=True)


def turn_two_kernel(owners, part, cot, mid, gains, g_in, g_out, new, full, tile_sum, p_in, p_out, *scratch):
    n = len(Reduce.scratch())
    bufs, ybufs, (gs, gr, rs, rr, ys, yr) = scratch[:n], scratch[n : n + 3], scratch[n + 3 :]
    z, x, c, y = place()
    greet(peers_near(True))
    r = Reduce(part, bufs, rs, rr)
    r.start_c()
    r.start_opposite()
    r.start_near()
    parts = (p_in, p_out)
    for m, g in enumerate((g_in, g_out)):
        dest = [slot_of(owners, m, k) for k in range(16)]

        def slot(q, _, g=g, p=parts[m], dest=dest):
            row, s = q // 3, q % 3
            total = jnp.zeros((64, 512), BF)
            for k in range(16):
                total = total + g[k] * ones_if(dest[k] == q)
            p[row // 4, row % 4, pl.ds(pl.multiple_of(s * 64, 64), 64), :] = total
            return 0

        lax.fori_loop(0, 24, slot, 0)
    yr_ = YReduce(parts, 192, ybufs, ys, yr)
    yr_.start()
    r.finish_near()
    r.start_z()
    total = r.total()
    f = mid[...].astype(F32)
    new[...] = before_input(f, inv_rms(f), total * gains[1:2, :], cot[...].astype(F32)).astype(BF)
    g = Gather(new, full, gs, gr)
    g.start_z()
    yr_.middle()
    r.drain()
    g.start_x()
    g.forward_x()
    yr_.finish()
    for m in range(2):
        for h in range(2):
            for s in range(0, 192, 32):
                rows = pl.ds(s, 32)
                tile_sum[m, h, rows, :] = yr_.total(m, h, rows).astype(BF)
    g.finish()
    yr_.drain()


def turn_two(*args):
    out = (shape(16, 1024), shape(1024, 1024), shape(2, 2, 192, 512))
    scratch = [pltpu.VMEM((2, 4, 192, 512), BF)] * 2 + Reduce.scratch() + YReduce.scratch(192) + [
        DMA((Gather.sems,)), DMA((Gather.sems,)), DMA((Reduce.sems,)), DMA((Reduce.sems,)), DMA((12,)), DMA((12,)),
    ]
    return comm_call(turn_two_kernel, "turn_two", 2, out, scratch, [SM] + [VM] * 6, args)


def closing_kernel(
    part_two, part_one, g_in, g_out, tokens, mid, grad_mid, gains, tile_sum,
    hidden_out, grad_tokens, rbuf, tile_grad, sbuf, tile_got, *scratch,
):
    n = len(Reduce.scratch())
    bufs_a, bufs_b, ybufs = scratch[:n], scratch[n : 2 * n], scratch[2 * n : 2 * n + 3]
    rs, rr, ys, yr, ws, wr, ps, pr = scratch[2 * n + 3 :]
    zh = at("zh")
    greet_all()
    red = YReduce((g_in, g_out), 128, ybufs, ys, yr)
    red.start()
    a = Reduce(part_one, bufs_a, rs.at[0], rr.at[0])
    b = Reduce(part_two, bufs_b, rs.at[1], rr.at[1])
    for r in (a, b):
        r.start_c()
    pairs = [
        rcopy(tile_sum.at[m, 1 - zh], tile_got.at[m], ps.at[m], pr.at[m], {"zh": 1 - zh}) for m in range(2)
    ]
    for r in (a, b):
        r.start_opposite()
    for r in (a, b):
        r.start_near()
    red.middle()
    for r in (a, b):
        r.finish_near()
    for r in (a, b):
        r.start_z()
    red.finish()
    for h in range(2):
        def tile(q, _):
            rows = pl.ds(pl.multiple_of(q * 16, 16), 16)
            t = [red.total(m, h, rows) for m in range(2)]
            for i in range(4):
                sbuf[h * 32 + q * 4 + i] = jnp.concatenate(
                    [t[0][4 * i : 4 * i + 4], t[1][4 * i : 4 * i + 4]], axis=0
                ).astype(BF)
            return 0

        lax.fori_loop(0, 8, tile, 0)
    exchange_start(sbuf, rbuf, ws, wr)
    for m, cp in enumerate(pairs):
        cp.wait_recv()
        tile_grad[m, :, half(zh)] = tile_sum[m, zh]
        tile_grad[m, :, half(1 - zh)] = tile_got[m]
    f = tokens[...].astype(F32)
    grad_tokens[...] = before_input(f, inv_rms(f), a.total() * gains[0:1, :], grad_mid[...].astype(F32)).astype(BF)
    hidden_out[...] = (mid[...].astype(F32) + b.total()).astype(BF)
    exchange_wait(sbuf, rbuf, ws, wr)
    exchange_sent(sbuf, ws)
    a.drain()
    b.drain()
    red.drain()
    for cp in pairs:
        cp.wait_send()


def closing(*args):
    out = (shape(16, 1024), shape(16, 1024), shape(64, 8, 512), shape(2, 192, 1024))
    scratch = [pltpu.VMEM((64, 8, 512), BF), pltpu.VMEM((2, 192, 512), BF)]
    scratch += Reduce.scratch() * 2 + YReduce.scratch(128) + [
        DMA((2, Reduce.sems)), DMA((2, Reduce.sems)), DMA((12,)), DMA((12,)), DMA, DMA, DMA((2,)), DMA((2,)),
    ]
    return comm_call(closing_kernel, "closing", 3, out, scratch, [VM] * 9, args)


def adam_kernel(
    owners, rbuf, tile_grad, f_in, f_out, fm, fv, t_in, t_out, tm, tv,
    nf_in, nf_out, nfm, nfv, nt_in, nt_out, ntm, ntv, wide,
):
    d = pl.program_id(0)

    @pl.when(d == 0)
    def _():
        for q in range(4):
            wide[q] = rbuf[:, :, q * 128 : (q + 1) * 128].astype(F32).reshape(512, 128)

    row = at("zh") * 4 + at("y")
    for m, (w, nw) in enumerate(((f_in, nf_in), (f_out, nf_out))):
        for h in range(2):
            for q in range(4):
                cols = slice(h * 512 + q * 128, h * 512 + q * 128 + 128)
                grad = wide[q, pl.ds(h * 256 + m * 4 + d, 32, stride=8), :]
                w1, m1, v1 = adam_update(w[:, cols], grad, fm[m, :, cols], fv[m, :, cols])
                nw[:, cols] = w1
                nfm[m, :, cols] = m1
                nfv[m, :, cols] = v1
    for m, (w, nw) in enumerate(((t_in, nt_in), (t_out, nt_out))):
        count = jnp.int32(0)
        for k in range(16):
            count = count + jnp.where(owners[m, k] == row, 1, 0)
        for i in range(3):
            rows = slice(16 * i, 16 * i + 16)
            at_row = lax.broadcasted_iota(jnp.int32, (16, 1024), 0) + (d * 48 + 16 * i)
            keep = at_row < count * 64
            w0, m0, v0 = w[rows, :], tm[m, rows, :], tv[m, rows, :]
            w1, m1, v1 = adam_update(w0, tile_grad[m, rows, :].astype(F32), m0, v0)
            nw[rows, :] = jnp.where(keep, w1.astype(F32), w0.astype(F32)).astype(BF)
            ntm[m, rows, :] = jnp.where(keep, m1, m0)
            ntv[m, rows, :] = jnp.where(keep, v1, v0)


def adam(*args):
    flat = pl.BlockSpec((32, 1024), lambda d: (d, 0))
    tile = pl.BlockSpec((48, 1024), lambda d: (d, 0))
    flats = pl.BlockSpec((2, 32, 1024), lambda d: (0, d, 0))
    tiles = pl.BlockSpec((2, 48, 1024), lambda d: (0, d, 0))
    state = [flat, flat, flats, flats, tile, tile, tiles, tiles]
    return pl.pallas_call(
        adam_kernel,
        name="adam",
        grid=(4,),
        out_shape=(
            shape(128, 1024), shape(128, 1024), shape(2, 128, 1024, kind=F32), shape(2, 128, 1024, kind=F32),
            shape(192, 1024), shape(192, 1024), shape(2, 192, 1024, kind=F32), shape(2, 192, 1024, kind=F32),
        ),
        in_specs=[SM, VM, tiles] + state,
        out_specs=tuple(state),
        scratch_shapes=[pltpu.VMEM((4, 512, 128), F32)],
        cost_estimate=pl.CostEstimate(flops=4_000_000_000, bytes_accessed=13 * 2**20, transcendentals=0),
    )(*args)


def dot(a, b, dims, kind=F32):
    return lax.dot_general(a, b, (dims, ((), ())), preferred_element_type=F32).astype(kind)


def shards(
    tokens, grad_out, gains, flat_in, flat_out, flat_moment, flat_second,
    tile_in, tile_out, tile_moment, tile_second, owners,
):
    own = owners[:, 0, :]
    flat = jnp.stack([flat_in.reshape(4, 32, 2, 512), flat_out.reshape(4, 32, 2, 512)])
    sbuf = flat.transpose(3, 2, 0, 1, 4).reshape(64, 8, 512)
    normed_one, cot_two, w_in_one, w_out_one, pair = opening(tokens, grad_out, gains, sbuf, tile_in[0], tile_out[0])
    w_in_one, w_out_one = w_in_one.reshape(1024, 512), w_out_one.reshape(1024, 512)

    hidden_one = dot(normed_one, w_in_one, ((1,), (0,)))
    act_one = gelu_value(hidden_one).astype(BF)
    part = dot(act_one, w_out_one, ((1,), (1,)), BF)
    middle, normed_two, w_in_two, w_out_two = turn_one(own, part, tokens, gains, pair.reshape(2, 2, 192, 512))

    hidden_two = dot(normed_two, w_in_two, ((1,), (0,)))
    act_two = gelu_value(hidden_two).astype(BF)
    d_act_two = dot(cot_two, w_out_two, ((1,), (0,)))
    d_hidden_two = (d_act_two * gelu_slope(hidden_two)).astype(BF)
    part = dot(d_hidden_two, w_in_two, ((1,), (1,)), BF)
    grad_in_two = dot(normed_two, d_hidden_two, ((0,), (0,)), BF).reshape(16, 64, 512)
    grad_out_two = dot(cot_two, act_two, ((0,), (0,)), BF).reshape(16, 64, 512)
    grad_mid, cot_one, tile_sum = turn_two(own, part, grad_out, middle, gains, grad_in_two, grad_out_two)
    part_two = dot(act_two, w_out_two, ((1,), (1,)), BF)

    d_act_one = dot(cot_one, w_out_one, ((1,), (0,)))
    d_hidden_one = (d_act_one * gelu_slope(hidden_one)).astype(BF)
    part = dot(d_hidden_one, w_in_one, ((1,), (1,)), BF)
    grad_in_one = dot(normed_one, d_hidden_one, ((0,), (0,)), BF).reshape(2, 4, 128, 512)
    grad_out_one = dot(cot_one, act_one, ((0,), (0,)), BF).reshape(2, 4, 128, 512)
    hidden_out, grad_tokens, rbuf, tile_grad = closing(
        part_two, part, grad_in_one, grad_out_one, tokens, middle, grad_mid, gains, tile_sum
    )
    tile, tiles = (192, 1024), (2, 192, 1024)
    outs = adam(
        own, rbuf, tile_grad, flat_in, flat_out, flat_moment, flat_second,
        tile_in.reshape(tile), tile_out.reshape(tile), tile_moment.reshape(tiles), tile_second.reshape(tiles),
    )
    return (
        hidden_out, grad_tokens, *outs[:4], outs[4].reshape(tile_in.shape), outs[5].reshape(tile_in.shape),
        outs[6].reshape(tile_moment.shape), outs[7].reshape(tile_moment.shape),
    )


def solution(mesh):
    mesh = Mesh(mesh.devices.reshape(2, 4, 4, 4, 2), ALL)
    whole = P(ALL, None)
    state = P(None, ALL, None)
    tile = P(COL, ROW, None, None)
    tile_state = P(None, COL, ROW, None, None)
    return jax.shard_map(
        shards,
        mesh=mesh,
        in_specs=(whole, whole, P(), whole, whole, state, state, tile, tile, tile_state, tile_state, P(None, COL, None)),
        out_specs=(whole, whole, whole, whole, state, state, tile, tile, tile_state, tile_state),
        check_vma=False,
    )
```

```python
import functools

import jax
import jax.numpy as jnp
from jax import lax
from jax.experimental import pallas as pl
from jax.experimental.pallas import tpu as pltpu
from jax.sharding import Mesh, PartitionSpec as P

norm_eps = 1e-06
beta_one = 0.9
beta_two = 0.95
learn_rate = 0.002
decay_rate = 0.1
adam_eps = 1e-08
gelu_coef = 0.7978845608

ALL = ("zh", "y", "zl", "x", "c")
ROW = ("zh", "y")
COL = ("zl", "x", "c")
MESH = pl.DeviceIdType.MESH
BF = jnp.bfloat16
F32 = jnp.float32

def gelu_value(hidden):
    tanh_term = jnp.tanh(gelu_coef * (hidden + 0.044715 * hidden * hidden * hidden))
    return 0.5 * hidden * (1.0 + tanh_term)


def gelu_slope(hidden):
    tanh_term = jnp.tanh(gelu_coef * (hidden + 0.044715 * hidden * hidden * hidden))
    return 0.5 * (1.0 + tanh_term) + 0.5 * hidden * (1.0 - tanh_term * tanh_term) * gelu_coef * (
        1.0 + 0.134145 * hidden * hidden
    )


def adam_update(weight, gradient, moment, second):
    new_moment = beta_one * moment + (1.0 - beta_one) * gradient
    new_second = beta_two * second + (1.0 - beta_two) * gradient * gradient
    weight_float = weight.astype(jnp.float32)
    stepped = weight_float - learn_rate * (
        new_moment / (jnp.sqrt(new_second) + adam_eps) + decay_rate * weight_float
    )
    return (stepped.astype(jnp.bfloat16), new_moment, new_second)


def dev_z(z):
    return {"zh": z // 4, "zl": z % 4}


def at(a):
    return lax.axis_index(a)


def place():
    return at("zh") * 4 + at("zl"), at("x"), at("c"), at("y")


def flat_dev(t):
    return {"zh": t // 32, "zl": (t // 8) % 4, "x": (t // 2) % 4, "c": t % 2}


def my_flat():
    z, x, c, _ = place()
    return z * 8 + x * 2 + c


def greet_all():
    me = my_flat()
    y = at("y")
    sem = pltpu.get_barrier_semaphore()

    def one(o, _):
        pl.semaphore_signal(sem, inc=1, device_id=flat_dev((me + o) % 64), device_id_type=MESH)
        return 0

    lax.fori_loop(1, 64, one, 0)
    for d in (1, 3):
        pl.semaphore_signal(sem, inc=1, device_id={"y": (y + d) % 4}, device_id_type=MESH)
    pl.semaphore_wait(sem, 65)


def rcopy(src, dst, ssem, rsem, dev):
    cp = pltpu.make_async_remote_copy(
        src_ref=src, dst_ref=dst, send_sem=ssem, recv_sem=rsem, device_id=dev, device_id_type=MESH
    )
    cp.start()
    return cp


def exchange_start(sbuf, rbuf, ssem, rsem):
    me = my_flat()

    def one(o, _):
        t = (me + o) % 64
        rcopy(sbuf.at[t], rbuf.at[me], ssem, rsem, flat_dev(t))
        return 0

    lax.fori_loop(1, 64, one, 0)
    rbuf[me] = sbuf[me]


def exchange_wait(sbuf, rbuf, ssem, rsem):
    part = pltpu.make_async_copy(rbuf.at[pl.ds(0, 63)], rbuf.at[pl.ds(0, 63)], rsem)
    part.wait()


def exchange_sent(sbuf, ssem):
    part = pltpu.make_async_copy(sbuf.at[pl.ds(0, 63)], sbuf.at[pl.ds(0, 63)], ssem)
    part.wait()


def blk(c, x, n=128, off=0):
    return pl.ds(pl.multiple_of(c * 512 + x * 128 + off, 16), n)


class Gather:
    sems = 7 + 2 + 2 + 4

    def __init__(self, own, full, ss, rs):
        self.own, self.full, self.ss, self.rs = own, full, ss, rs

    def start_z(self):
        z, x, c, _ = place()
        mine = blk(c, x, 16, z * 16)
        self.sent = []
        self.zc = [
            rcopy(self.own, self.full.at[mine], self.ss.at[d - 1], self.rs.at[d - 1], dev_z((z + d) % 8))
            for d in range(1, 8)
        ]
        self.full[mine, :] = self.own[...]

    def move(self, rows, k, dev):
        ref = self.full.at[rows]
        cp = rcopy(ref, ref, self.ss.at[k], self.rs.at[k], dev)
        self.sent.append(cp)
        return cp

    def start_x(self):
        z, x, c, _ = place()
        for cp in self.zc:
            cp.wait_recv()
        self.right = self.move(blk(c, x), 7, {"x": (x + 1) % 4})
        self.left = self.move(blk(c, x), 8, {"x": (x + 3) % 4})
        self.cores = [self.move(blk(c, x), 11, {"c": 1 - c})]

    def right_in(self):
        z, x, c, _ = place()
        self.right.wait_recv()
        self.fr = self.move(blk(c, (x + 3) % 4, 64), 9, {"x": (x + 1) % 4})
        self.cores.append(self.move(blk(c, (x + 3) % 4), 12, {"c": 1 - c}))

    def left_in(self):
        z, x, c, _ = place()
        self.left.wait_recv()
        self.fl = self.move(blk(c, (x + 1) % 4, 64, 64), 10, {"x": (x + 3) % 4})
        self.cores.append(self.move(blk(c, (x + 1) % 4), 13, {"c": 1 - c}))

    def far_in(self):
        z, x, c, _ = place()
        self.fr.wait_recv()
        self.fl.wait_recv()
        self.cores.append(self.move(blk(c, (x + 2) % 4), 14, {"c": 1 - c}))

    def cores_in(self):
        for cp in self.cores:
            cp.wait_recv()

    def drain(self):
        for cp in self.zc + self.sent:
            cp.wait_send()


def add_rows(dst, dst_at, terms, rows, step=32):
    for r in range(0, rows, step):
        total = None
        for ref, base in terms:
            v = ref[pl.ds(base + r, step), :].astype(F32)
            total = v if total is None else total + v
        dst[pl.ds(dst_at + r, step), :] = total.astype(dst.dtype)


class Reduce:
    sems = 4 + 2 + 4 + 7

    @staticmethod
    def scratch():
        return [
            pltpu.VMEM((512, 1024), BF),
            pltpu.VMEM((128, 1024), BF),
            pltpu.VMEM((128, 1024), BF),
            pltpu.VMEM((256, 1024), BF),
            pltpu.VMEM((256, 1024), BF),
            pltpu.VMEM((128, 1024), BF),
            pltpu.VMEM((112, 1024), BF),
        ]

    def __init__(self, part, bufs, ss, rs):
        self.part, self.ss, self.rs = part, ss, rs
        self.crecv, self.obuf, self.orecv, self.nbuf, self.xrecv, self.zbuf, self.zrecv = bufs
        self.sent = []

    def send(self, src, dst, k, dev):
        cp = rcopy(src, dst, self.ss.at[k], self.rs.at[k], dev)
        self.sent.append(cp)
        return cp

    def start_c(self):
        z, x, c, _ = place()
        self.cores = []
        for k, d in enumerate((2, 1, 3, 0)):
            xx = (x + d) % 4
            self.cores.append(
                self.send(
                    self.part.at[blk(1 - c, xx)],
                    self.crecv.at[pl.ds(pl.multiple_of(xx * 128, 128), 128)],
                    k,
                    {"c": 1 - c},
                )
            )

    def start_opposite(self):
        z, x, c, _ = place()
        self.cores[0].wait_recv()
        o = (x + 2) % 4
        terms = [(self.part, c * 512 + o * 128), (self.crecv, o * 128)]
        add_rows(self.obuf, 0, terms, 128)
        half = pl.ds(0, 64)
        rest = pl.ds(64, 64)
        self.o_right = self.send(self.obuf.at[half], self.orecv.at[half], 4, {"x": (x + 1) % 4})
        self.o_left = self.send(self.obuf.at[rest], self.orecv.at[rest], 5, {"x": (x + 3) % 4})

    def start_near(self):
        z, x, c, _ = place()
        r, l = (x + 1) % 4, (x + 3) % 4
        self.near = []
        self.cores[1].wait_recv()
        add_rows(self.nbuf, 64, [(self.part, c * 512 + r * 128 + 64), (self.crecv, r * 128 + 64)], 64)
        s = pl.ds(64, 64)
        self.near.append(self.send(self.nbuf.at[s], self.xrecv.at[s], 6, {"x": r}))
        self.cores[2].wait_recv()
        add_rows(self.nbuf, 128, [(self.part, c * 512 + l * 128), (self.crecv, l * 128)], 64)
        s = pl.ds(128, 64)
        self.near.append(self.send(self.nbuf.at[s], self.xrecv.at[s], 7, {"x": l}))

    def finish_near(self):
        z, x, c, _ = place()
        r, l = (x + 1) % 4, (x + 3) % 4
        self.o_right.wait_recv()
        add_rows(
            self.nbuf, 0,
            [(self.part, c * 512 + r * 128), (self.crecv, r * 128), (self.orecv, 0)], 64,
        )
        s = pl.ds(0, 64)
        self.near.append(self.send(self.nbuf.at[s], self.xrecv.at[s], 8, {"x": r}))
        self.o_left.wait_recv()
        add_rows(
            self.nbuf, 192,
            [(self.part, c * 512 + l * 128 + 64), (self.crecv, l * 128 + 64), (self.orecv, 64)], 64,
        )
        s = pl.ds(192, 64)
        self.near.append(self.send(self.nbuf.at[s], self.xrecv.at[s], 9, {"x": l}))

    def start_z(self):
        z, x, c, _ = place()
        self.cores[3].wait_recv()
        for cp in self.near:
            cp.wait_recv()
        terms = [(self.part, c * 512 + x * 128), (self.crecv, x * 128), (self.xrecv, 0), (self.xrecv, 128)]
        add_rows(self.zbuf, 0, terms, 128)
        self.zc = []
        for d in range(1, 8):
            t = (z + d) % 8
            src = self.zbuf.at[pl.ds(pl.multiple_of(t * 16, 16), 16)]
            self.zc.append(self.send(src, self.zrecv.at[pl.ds((d - 1) * 16, 16)], 9 + d, dev_z(t)))

    def total(self):
        z, x, c, _ = place()
        out = self.zbuf[pl.ds(pl.multiple_of(z * 16, 16), 16), :].astype(F32)
        for d in range(1, 8):
            self.zc[d - 1].wait_recv()
            out = out + self.zrecv[pl.ds((d - 1) * 16, 16), :].astype(F32)
        return out

    def drain(self):
        for cp in self.sent:
            cp.wait_send()


class YGather:
    def __init__(self, own, full, ss, rs):
        self.own, self.full, self.ss, self.rs = own, full, ss, rs

    def copy(self, src, m, h, yy, k, dev):
        return rcopy(src, self.full[m].at[h, yy], self.ss.at[k], self.rs.at[k], dev)

    def start(self):
        y = at("y")
        self.up, self.down = {"y": (y + 1) % 4}, {"y": (y + 3) % 4}
        self.ups, self.downs = {}, {}
        for h in range(2):
            for m in range(2):
                self.ups[h, m] = self.copy(self.own(m, h), m, h, y, h * 2 + m, self.up)
        for h in (1, 0):
            for m in range(2):
                self.downs[h, m] = self.copy(self.own(m, h), m, h, y, 4 + h * 2 + m, self.down)

    def forward(self):
        y = at("y")
        self.far = []
        for m in range(2):
            self.ups[0, m].wait_recv()
            yy = (y + 3) % 4
            self.far.append(self.copy(self.full[m].at[0, yy], m, 0, yy, 8 + m, self.up))
            self.downs[1, m].wait_recv()
            yy = (y + 1) % 4
            self.far.append(self.copy(self.full[m].at[1, yy], m, 1, yy, 10 + m, self.down))

    def finish(self):
        for m in range(2):
            self.ups[1, m].wait_recv()
            self.downs[0, m].wait_recv()
        for cp in self.far:
            cp.wait_recv()

    def drain(self):
        for cp in self.far + list(self.ups.values()) + list(self.downs.values()):
            cp.wait_send()


class YReduce:
    @staticmethod
    def scratch(rows):
        return [
            pltpu.VMEM((2, 2, rows, 512), BF),
            pltpu.VMEM((2, 2, rows, 512), BF),
            pltpu.VMEM((2, 2, 2, rows, 512), BF),
        ]

    def __init__(self, part, rows, bufs, ss, rs):
        self.part, self.rows, self.ss, self.rs = part, rows, ss, rs
        self.orv, self.nh, self.xin = bufs
        y = at("y")
        self.up, self.down = {"y": (y + 1) % 4}, {"y": (y + 3) % 4}
        self.opp, self.plain, self.mixed = {}, [], []

    def copy(self, src, dst, k, dev):
        return rcopy(src, dst, self.ss.at[k], self.rs.at[k], dev)

    def start(self, m):
        y = at("y")
        u, d, o = (y + 1) % 4, (y + 3) % 4, (y + 2) % 4
        self.opp[m, 0] = self.copy(self.part[m].at[0, o], self.orv.at[m, 0], m, self.up)
        self.opp[m, 1] = self.copy(self.part[m].at[1, o], self.orv.at[m, 1], 2 + m, self.down)
        self.plain.append(self.copy(self.part[m].at[1, u], self.xin.at[m, 0, 1], 4 + m, self.up))
        self.plain.append(self.copy(self.part[m].at[0, d], self.xin.at[m, 1, 0], 6 + m, self.down))

    def middle(self, m):
        y = at("y")
        u, d = (y + 1) % 4, (y + 3) % 4
        for h, yy, dev in ((0, u, self.up), (1, d, self.down)):
            self.opp[m, h].wait_recv()
            for s in range(0, self.rows, 32):
                self.nh[m, h, s : s + 32, :] = (
                    self.part[m][h, yy, s : s + 32, :].astype(F32) + self.orv[m, h, s : s + 32, :].astype(F32)
                ).astype(BF)
            self.mixed.append(self.copy(self.nh.at[m, h], self.xin.at[m, h, h], 8 + 2 * h + m, dev))

    def finish(self):
        for cp in self.plain + self.mixed:
            cp.wait_recv()

    def total(self, m, h, rows):
        return (
            self.part[m][h, at("y"), rows, :].astype(F32)
            + self.xin[m, 0, h, rows, :].astype(F32)
            + self.xin[m, 1, h, rows, :].astype(F32)
        )

    def drain(self):
        for cp in list(self.opp.values()) + self.plain + self.mixed:
            cp.wait_send()


def inv_rms(f):
    return lax.rsqrt(jnp.mean(f * f, axis=1, keepdims=True) + norm_eps)


def slot_of(owners, m, k):
    own, rank = owners[m, k], jnp.int32(0)
    for j in range(16):
        rank = rank + jnp.where((owners[m, j] == own) & (j < k), 1, 0)
    return own * 3 + rank


def ones_if(hit):
    return jnp.full((64, 512), jnp.where(hit, 1.0, 0.0), F32).astype(BF)


def half(h):
    return pl.ds(pl.multiple_of(h * 512, 128), 512)


VM = pl.BlockSpec(memory_space=pltpu.VMEM)
SM = pl.BlockSpec(memory_space=pltpu.SMEM)
DMA = pltpu.SemaphoreType.DMA


def comm_call(kernel, name, ident, out_shape, scratch, in_specs, args):
    return pl.pallas_call(
        kernel,
        name=name,
        out_shape=out_shape,
        in_specs=in_specs,
        out_specs=(VM,) * len(out_shape),
        scratch_shapes=scratch,
        compiler_params=pltpu.CompilerParams(collective_id=ident, has_side_effects=True, vmem_limit_bytes=67_043_328),
        cost_estimate=pl.CostEstimate(flops=40_000_000_000, bytes_accessed=2**23, transcendentals=0),
    )(*args)


def shape(*dims, kind=BF):
    return jax.ShapeDtypeStruct(dims, kind)


def before_input(f, inv, gated, base):
    return base + inv * gated - f * inv * inv * inv * jnp.mean(f * gated, axis=1, keepdims=True)


def full(w):
    return w[...].reshape(1024, 512)


def mul(a, b, dims):
    return lax.dot_general(a, b, (dims, ((), ())), preferred_element_type=F32)


def up(rows, src, w_in, hid, act):
    h = mul(src[rows, :], full(w_in), ((1,), (0,)))
    hid[rows, :] = h
    act[rows, :] = gelu_value(h).astype(BF)


def down(rows, cot, w_out, hid, dh):
    d = mul(cot[rows, :], full(w_out), ((1,), (0,)))
    dh[rows, :] = (d * gelu_slope(hid[rows, :])).astype(BF)


def back(rows, src, w, part):
    part[rows, :] = mul(src[rows, :], full(w), ((1,), (1,))).astype(BF)


def outer(left, right, store):
    for i in range(4):
        store(i, mul(left[:, i * 256 : (i + 1) * 256], right[...], ((0,), (0,))).astype(BF))


def as_flat(ref):
    def store(i, v):
        ref[i // 2, (i % 2) * 2] = v[:128]
        ref[i // 2, (i % 2) * 2 + 1] = v[128:]

    return store


def as_tiles(ref):
    def store(i, v):
        ref[i * 4 : (i + 1) * 4] = v.reshape(4, 64, 512)

    return store


def pick_tiles(owners, m, slots, w):
    def tile(k, _):
        want = slot_of(owners, m, k)
        total = jnp.zeros((64, 512), BF)
        for q in range(24):
            r, s = q // 3, q % 3
            total = total + slots[r // 4, r % 4, s * 64 : (s + 1) * 64, :] * ones_if(want == q)
        w[k] = total
        return 0

    lax.fori_loop(0, 16, tile, 0)


def place_tiles(owners, m, g, p):
    dest = [slot_of(owners, m, k) for k in range(16)]

    def slot(q, _):
        row, s = q // 3, q % 3
        total = jnp.zeros((64, 512), BF)
        for k in range(16):
            total = total + g[k] * ones_if(dest[k] == q)
        p[row // 4, row % 4, pl.ds(pl.multiple_of(s * 64, 64), 64), :] = total
        return 0

    lax.fori_loop(0, 24, slot, 0)


def scratch_of():
    vm = pltpu.VMEM
    tok, wt, act, f32 = vm((1024, 1024), BF), vm((2, 4, 128, 512), BF), vm((1024, 512), BF), vm((1024, 512), F32)
    tiles, slots, flat = vm((16, 64, 512), BF), vm((2, 4, 192, 512), BF), vm((64, 8, 512), BF)
    own, n, k = vm((16, 1024), BF), Gather.sems, Reduce.sems
    named = dict(
        normed_one=tok, normed_two=tok, cot_two=tok, cot_one=tok, part_a=tok, part_b=tok,
        w_in_one=wt, w_out_one=wt, w_in_two=tiles, w_out_two=tiles, hid_one=f32, hid_two=f32, act_one=act, act_two=act, dh=act,
        pair=vm((2, 2, 192, 512), BF), rbuf_w=flat, s_in=slots, s_out=slots, gt_in=tiles, gt_out=tiles, p_in=slots, p_out=slots,
        gf_in=wt, gf_out=wt, sbuf_g=flat, tile_sum=vm((2, 2, 192, 512), BF), tile_got=vm((2, 192, 512), BF),
        own_one=own, own_two=own, mid=own, grad_mid=own,
        gs=DMA((4, n)), gr=DMA((4, n)), rs=DMA((4, k)), rr=DMA((4, k)), ys=DMA((4, 12)), yr=DMA((4, 12)),
        ws=DMA((2,)), wr=DMA((2,)), ps=DMA((4,)), pr=DMA((4,)),
    )
    reduces = [Reduce.scratch() for _ in range(3)]
    return named, reduces, YReduce.scratch(192), YReduce.scratch(128)


class Bag:
    pass


def step_kernel(owners, tokens, cot, gains, sbuf, t_in, t_out, hidden_out, grad_tokens, rbuf, tile_grad, *scratch):
    named, reduces, tile_y, flat_y = scratch_of()
    v, refs = Bag(), list(scratch)
    for name in named:
        setattr(v, name, refs.pop(0))
    bufs = []
    for r in reduces:
        bufs.append(refs[: len(r)])
        refs = refs[len(r) :]
    tile_bufs, flat_bufs = refs[:3], refs[3:]
    z, x, c, y = place()
    zh = at("zh")
    near = [blk(c, (x + d) % 4) for d in (0, 3, 1, 2)]
    far = [blk(1 - c, 0, 256), blk(1 - c, 2, 256)]

    f = tokens[...].astype(F32)
    v.own_one[...] = (f * inv_rms(f) * gains[0:1, :]).astype(BF)
    greet_all()
    exchange_start(sbuf, v.rbuf_w, v.ws.at[0], v.wr.at[0])
    a = Gather(v.own_one, v.normed_one, v.gs.at[0], v.gr.at[0])
    b = Gather(cot, v.cot_two, v.gs.at[1], v.gr.at[1])
    a.start_z()
    b.start_z()
    pairs = [
        rcopy(t.at[:, half(1 - zh)], v.pair.at[m, zh], v.ps.at[m], v.pr.at[m], {"zh": 1 - zh})
        for m, t in enumerate((t_in, t_out))
    ]
    for m, t in enumerate((t_in, t_out)):
        v.pair[m, zh] = t[:, half(zh)]
    exchange_wait(sbuf, v.rbuf_w, v.ws.at[0], v.wr.at[0])
    for h in range(2):
        def tile(q, _):
            got = [v.rbuf_w[h * 32 + q * 4 + i].astype(F32) for i in range(4)]
            rows = pl.ds(pl.multiple_of(q * 16, 16), 16)
            v.w_in_one[h, y, rows, :] = jnp.concatenate([u[0:4] for u in got], axis=0).astype(BF)
            v.w_out_one[h, y, rows, :] = jnp.concatenate([u[4:8] for u in got], axis=0).astype(BF)
            return 0

        lax.fori_loop(0, 8, tile, 0)
    ones = (v.w_in_one, v.w_out_one)
    yg = YGather(lambda m, h: ones[m].at[h, y], ones, v.ys.at[0], v.yr.at[0])
    yg.start()
    a.start_x()
    a.right_in()
    a.left_in()
    yg.forward()
    a.far_in()
    b.start_x()
    a.cores_in()
    yg.finish()

    for rows in far:
        up(rows, v.normed_one, v.w_in_one, v.hid_one, v.act_one)
        back(rows, v.act_one, v.w_out_one, v.part_a)
    r = Reduce(v.part_a, bufs[0], v.rs.at[0], v.rr.at[0])
    r.start_c()
    slots = (v.s_in, v.s_out)
    for cp in pairs:
        cp.wait_recv()
    yt = YGather(lambda m, h: v.pair.at[m, h], slots, v.ys.at[1], v.yr.at[1])
    yt.start()
    for i in range(2):
        rows = blk(c, 2 * i, 256)
        up(rows, v.normed_one, v.w_in_one, v.hid_one, v.act_one)
        back(rows, v.act_one, v.w_out_one, v.part_a)
    r.start_opposite()
    r.start_near()
    b.right_in()
    b.left_in()
    for m in range(2):
        for h in range(2):
            slots[m][h, y] = v.pair[m, h]
    r.finish_near()
    r.start_z()
    b.far_in()
    yt.forward()
    v.mid[...] = (tokens[...].astype(F32) + r.total()).astype(BF)
    f = v.mid[...].astype(F32)
    v.own_two[...] = (f * inv_rms(f) * gains[1:2, :]).astype(BF)
    a2 = Gather(v.own_two, v.normed_two, v.gs.at[2], v.gr.at[2])
    a2.start_z()
    r.drain()
    yt.finish()
    for m, w in enumerate((v.w_in_two, v.w_out_two)):
        pick_tiles(owners, m, slots[m], w)
    a2.start_x()
    b.cores_in()

    def layer_two(rows):
        up(rows, v.normed_two, v.w_in_two, v.hid_two, v.act_two)
        down(rows, v.cot_two, v.w_out_two, v.hid_two, v.dh)
        back(rows, v.dh, v.w_in_two, v.part_a)

    layer_two(near[0])
    a2.right_in()
    layer_two(near[1])
    a2.left_in()
    layer_two(near[2])
    a2.far_in()
    layer_two(near[3])
    a2.cores_in()
    for rows in far:
        layer_two(rows)
    r = Reduce(v.part_a, bufs[1], v.rs.at[1], v.rr.at[1])
    r.start_c()
    r.start_opposite()
    r.start_near()
    outer(v.normed_two, v.dh, as_tiles(v.gt_in))
    r.finish_near()
    outer(v.cot_two, v.act_two, as_tiles(v.gt_out))
    r.start_z()
    ty = YReduce((v.p_in, v.p_out), 192, tile_bufs, v.ys.at[2], v.yr.at[2])
    for m, (g, p) in enumerate(((v.gt_in, v.p_in), (v.gt_out, v.p_out))):
        place_tiles(owners, m, g, p)
        ty.start(m)
    f = v.mid[...].astype(F32)
    v.grad_mid[...] = before_input(f, inv_rms(f), r.total() * gains[1:2, :], cot[...].astype(F32)).astype(BF)
    b2 = Gather(v.grad_mid, v.cot_one, v.gs.at[3], v.gr.at[3])
    b2.start_z()
    r.drain()
    for i in range(4):
        back(pl.ds(i * 256, 256), v.act_two, v.w_out_two, v.part_b)
    s = Reduce(v.part_b, bufs[2], v.rs.at[2], v.rr.at[2])
    s.start_c()
    b2.start_x()
    s.start_opposite()
    s.start_near()

    def layer_one(rows):
        down(rows, v.cot_one, v.w_out_one, v.hid_one, v.dh)
        back(rows, v.dh, v.w_in_one, v.part_a)

    layer_one(near[0])
    b2.right_in()
    layer_one(near[1])
    b2.left_in()
    layer_one(near[2])
    for m in range(2):
        ty.middle(m)
    b2.far_in()
    layer_one(near[3])
    b2.cores_in()
    fy = YReduce((v.gf_in, v.gf_out), 128, flat_bufs, v.ys.at[3], v.yr.at[3])
    outer(v.cot_one, v.act_one, as_flat(v.gf_out))
    fy.start(1)
    for rows in far:
        down(rows, v.cot_one, v.w_out_one, v.hid_one, v.dh)
    outer(v.normed_one, v.dh, as_flat(v.gf_in))
    fy.start(0)
    for rows in far:
        back(rows, v.dh, v.w_in_one, v.part_a)
    r = Reduce(v.part_a, bufs[0], v.rs.at[3], v.rr.at[3])
    r.start_c()
    s.finish_near()
    r.start_opposite()
    r.start_near()
    ty.finish()
    for m in range(2):
        for h in range(2):
            for k in range(0, 192, 32):
                rows = pl.ds(k, 32)
                v.tile_sum[m, h, rows, :] = ty.total(m, h, rows).astype(BF)
    swaps = [
        rcopy(v.tile_sum.at[m, 1 - zh], v.tile_got.at[m], v.ps.at[2 + m], v.pr.at[2 + m], {"zh": 1 - zh})
        for m in range(2)
    ]
    fy.middle(1)
    fy.middle(0)
    s.start_z()
    r.finish_near()
    r.start_z()
    fy.finish()
    for h in range(2):
        def tile(q, _):
            rows = pl.ds(pl.multiple_of(q * 16, 16), 16)
            t = [fy.total(m, h, rows) for m in range(2)]
            for i in range(4):
                v.sbuf_g[h * 32 + q * 4 + i] = jnp.concatenate(
                    [t[0][4 * i : 4 * i + 4], t[1][4 * i : 4 * i + 4]], axis=0
                ).astype(BF)
            return 0

        lax.fori_loop(0, 8, tile, 0)
    exchange_start(v.sbuf_g, rbuf, v.ws.at[1], v.wr.at[1])
    for m, cp in enumerate(swaps):
        cp.wait_recv()
        tile_grad[m, :, half(zh)] = v.tile_sum[m, zh]
        tile_grad[m, :, half(1 - zh)] = v.tile_got[m]
    hidden_out[...] = (v.mid[...].astype(F32) + s.total()).astype(BF)
    f = tokens[...].astype(F32)
    grad_tokens[...] = before_input(f, inv_rms(f), r.total() * gains[0:1, :], v.grad_mid[...].astype(F32)).astype(BF)
    exchange_wait(v.sbuf_g, rbuf, v.ws.at[1], v.wr.at[1])
    exchange_sent(v.sbuf_g, v.ws.at[1])
    exchange_sent(sbuf, v.ws.at[0])
    for cp in pairs + swaps:
        cp.wait_send()
    for q in (a, b, a2, b2, yg, yt, ty, fy, r, s):
        q.drain()


def step(*args):
    named, reduces, tile_y, flat_y = scratch_of()
    out = (shape(16, 1024), shape(16, 1024), shape(64, 8, 512), shape(2, 192, 1024))
    scratch = list(named.values()) + sum(reduces, []) + tile_y + flat_y
    return comm_call(step_kernel, "step", 0, out, scratch, [SM] + [VM] * 6, args)


def adam_kernel(
    owners, rbuf, tile_grad, f_in, f_out, fm, fv, t_in, t_out, tm, tv,
    nf_in, nf_out, nfm, nfv, nt_in, nt_out, ntm, ntv, wide,
):
    d = pl.program_id(0)

    @pl.when(d == 0)
    def _():
        for q in range(4):
            wide[q] = rbuf[:, :, q * 128 : (q + 1) * 128].astype(F32).reshape(512, 128)

    row = at("zh") * 4 + at("y")
    for m, (w, nw) in enumerate(((f_in, nf_in), (f_out, nf_out))):
        for h in range(2):
            for q in range(4):
                cols = slice(h * 512 + q * 128, h * 512 + q * 128 + 128)
                grad = wide[q, pl.ds(h * 256 + m * 4 + d, 32, stride=8), :]
                w1, m1, v1 = adam_update(w[:, cols], grad, fm[m, :, cols], fv[m, :, cols])
                nw[:, cols] = w1
                nfm[m, :, cols] = m1
                nfv[m, :, cols] = v1
    for m, (w, nw) in enumerate(((t_in, nt_in), (t_out, nt_out))):
        count = jnp.int32(0)
        for k in range(16):
            count = count + jnp.where(owners[m, k] == row, 1, 0)
        for i in range(3):
            rows = slice(16 * i, 16 * i + 16)
            at_row = lax.broadcasted_iota(jnp.int32, (16, 1024), 0) + (d * 48 + 16 * i)
            keep = at_row < count * 64
            w0, m0, v0 = w[rows, :], tm[m, rows, :], tv[m, rows, :]
            w1, m1, v1 = adam_update(w0, tile_grad[m, rows, :].astype(F32), m0, v0)
            nw[rows, :] = jnp.where(keep, w1.astype(F32), w0.astype(F32)).astype(BF)
            ntm[m, rows, :] = jnp.where(keep, m1, m0)
            ntv[m, rows, :] = jnp.where(keep, v1, v0)


def adam(*args):
    flat = pl.BlockSpec((32, 1024), lambda d: (d, 0))
    tile = pl.BlockSpec((48, 1024), lambda d: (d, 0))
    flats = pl.BlockSpec((2, 32, 1024), lambda d: (0, d, 0))
    tiles = pl.BlockSpec((2, 48, 1024), lambda d: (0, d, 0))
    state = [flat, flat, flats, flats, tile, tile, tiles, tiles]
    return pl.pallas_call(
        adam_kernel,
        name="adam",
        grid=(4,),
        out_shape=(
            shape(128, 1024), shape(128, 1024), shape(2, 128, 1024, kind=F32), shape(2, 128, 1024, kind=F32),
            shape(192, 1024), shape(192, 1024), shape(2, 192, 1024, kind=F32), shape(2, 192, 1024, kind=F32),
        ),
        in_specs=[SM, VM, tiles] + state,
        out_specs=tuple(state),
        scratch_shapes=[pltpu.VMEM((4, 512, 128), F32)],
        cost_estimate=pl.CostEstimate(flops=4_000_000_000, bytes_accessed=13 * 2**20, transcendentals=0),
    )(*args)


def shards(
    tokens, grad_out, gains, flat_in, flat_out, flat_moment, flat_second,
    tile_in, tile_out, tile_moment, tile_second, owners,
):
    own = owners[:, 0, :]
    flat = jnp.stack([flat_in.reshape(4, 32, 2, 512), flat_out.reshape(4, 32, 2, 512)])
    sbuf = flat.transpose(3, 2, 0, 1, 4).reshape(64, 8, 512)
    tile, tiles = (192, 1024), (2, 192, 1024)
    hidden_out, grad_tokens, rbuf, tile_grad = step(
        own, tokens, grad_out, gains, sbuf, tile_in.reshape(tile), tile_out.reshape(tile)
    )
    outs = adam(
        own, rbuf, tile_grad, flat_in, flat_out, flat_moment, flat_second,
        tile_in.reshape(tile), tile_out.reshape(tile), tile_moment.reshape(tiles), tile_second.reshape(tiles),
    )
    return (
        hidden_out, grad_tokens, *outs[:4], outs[4].reshape(tile_in.shape), outs[5].reshape(tile_in.shape),
        outs[6].reshape(tile_moment.shape), outs[7].reshape(tile_moment.shape),
    )


def solution(mesh):
    mesh = Mesh(mesh.devices.reshape(2, 4, 4, 4, 2), ALL)
    whole = P(ALL, None)
    state = P(None, ALL, None)
    tile = P(COL, ROW, None, None)
    tile_state = P(None, COL, ROW, None, None)
    return jax.shard_map(
        shards,
        mesh=mesh,
        in_specs=(whole, whole, P(), whole, whole, state, state, tile, tile, tile_state, tile_state, P(None, COL, None)),
        out_specs=(whole, whole, whole, whole, state, state, tile, tile, tile_state, tile_state),
        check_vma=False,
    )
```

```python
import functools

import jax
import jax.numpy as jnp
from jax import lax
from jax.experimental import pallas as pl
from jax.experimental.pallas import tpu as pltpu
from jax.sharding import Mesh, PartitionSpec as P

norm_eps = 1e-06
beta_one = 0.9
beta_two = 0.95
learn_rate = 0.002
decay_rate = 0.1
adam_eps = 1e-08
gelu_coef = 0.7978845608

ALL = ("zh", "y", "zl", "x", "c")
ROW = ("zh", "y")
COL = ("zl", "x", "c")
MESH = pl.DeviceIdType.MESH
BF = jnp.bfloat16
F32 = jnp.float32

def gelu_value(hidden):
    tanh_term = jnp.tanh(gelu_coef * (hidden + 0.044715 * hidden * hidden * hidden))
    return 0.5 * hidden * (1.0 + tanh_term)


def gelu_slope(hidden):
    tanh_term = jnp.tanh(gelu_coef * (hidden + 0.044715 * hidden * hidden * hidden))
    return 0.5 * (1.0 + tanh_term) + 0.5 * hidden * (1.0 - tanh_term * tanh_term) * gelu_coef * (
        1.0 + 0.134145 * hidden * hidden
    )


def adam_update(weight, gradient, moment, second):
    new_moment = beta_one * moment + (1.0 - beta_one) * gradient
    new_second = beta_two * second + (1.0 - beta_two) * gradient * gradient
    weight_float = weight.astype(jnp.float32)
    stepped = weight_float - learn_rate * (
        new_moment / (jnp.sqrt(new_second) + adam_eps) + decay_rate * weight_float
    )
    return (stepped.astype(jnp.bfloat16), new_moment, new_second)


def dev_z(z):
    return {"zh": z // 4, "zl": z % 4}


def at(a):
    return lax.axis_index(a)


def place():
    return at("zh") * 4 + at("zl"), at("x"), at("c"), at("y")


def flat_dev(t):
    return {"zh": t // 32, "zl": (t // 8) % 4, "x": (t // 2) % 4, "c": t % 2}


def my_flat():
    z, x, c, _ = place()
    return z * 8 + x * 2 + c


def greet_all(meanwhile):
    me = my_flat()
    y = at("y")
    sem = pltpu.get_barrier_semaphore()

    def one(o, _):
        pl.semaphore_signal(sem, inc=1, device_id=flat_dev((me + o) % 64), device_id_type=MESH)
        return 0

    lax.fori_loop(1, 64, one, 0)
    for d in (1, 3):
        pl.semaphore_signal(sem, inc=1, device_id={"y": (y + d) % 4}, device_id_type=MESH)
    meanwhile()
    pl.semaphore_wait(sem, 65)


def rcopy(src, dst, ssem, rsem, dev):
    cp = pltpu.make_async_remote_copy(
        src_ref=src, dst_ref=dst, send_sem=ssem, recv_sem=rsem, device_id=dev, device_id_type=MESH
    )
    cp.start()
    return cp


def exchange_start(sbuf, rbuf, ssem, rsem):
    me = my_flat()

    def one(o, _):
        t = (me + o) % 64
        rcopy(sbuf.at[t], rbuf.at[me], ssem, rsem, flat_dev(t))
        return 0

    lax.fori_loop(1, 64, one, 0)
    rbuf[me] = sbuf[me]


def exchange_wait(sbuf, rbuf, ssem, rsem):
    part = pltpu.make_async_copy(rbuf.at[pl.ds(0, 63)], rbuf.at[pl.ds(0, 63)], rsem)
    part.wait()


def exchange_sent(sbuf, ssem):
    part = pltpu.make_async_copy(sbuf.at[pl.ds(0, 63)], sbuf.at[pl.ds(0, 63)], ssem)
    part.wait()


def blk(c, x, n=128, off=0):
    return pl.ds(pl.multiple_of(c * 512 + x * 128 + off, 16), n)


PIECES = (0, 1, 7, 2, 6, 3, 5, 4)


class Gather:
    sems = 7 + 16 + 8 + 4

    def __init__(self, own, full, ss, rs):
        self.own, self.full, self.ss, self.rs = own, full, ss, rs
        z, x, c, _ = place()
        self.right_dev, self.left_dev, self.core_dev = {"x": (x + 1) % 4}, {"x": (x + 3) % 4}, {"c": 1 - c}
        self.sent, self.right, self.left, self.far, self.cores = [], [], [], [], []

    def piece(self, xx, d):
        z, x, c, _ = place()
        return blk(c, xx, 16, (z + 8 - d) % 8 * 16)

    def send(self, src, rows, k, dev):
        cp = rcopy(src, self.full.at[rows], self.ss.at[k], self.rs.at[k], dev)
        self.sent.append(cp)
        return cp

    def pass_on(self, rows, k, dev):
        return self.send(self.full.at[rows], rows, k, dev)

    def start_z(self):
        z, x, c, _ = place()
        mine = self.piece(x, 0)
        self.zc = {d: self.send(self.own, mine, d - 1, dev_z((z + d) % 8)) for d in PIECES[1:]}
        self.right.append(self.send(self.own, mine, 7, self.right_dev))
        self.left.append(self.send(self.own, mine, 15, self.left_dev))
        self.full[mine, :] = self.own[...]

    def start_x(self):
        z, x, c, _ = place()
        for k in range(1, 8):
            d = PIECES[k]
            self.zc[d].wait_recv()
            self.right.append(self.pass_on(self.piece(x, d), 7 + k, self.right_dev))
            self.left.append(self.pass_on(self.piece(x, d), 15 + k, self.left_dev))
        self.cores.append(self.pass_on(blk(c, x), 31, self.core_dev))

    def sides_in(self):
        z, x, c, _ = place()
        for k in range(8):
            d = PIECES[k]
            self.right[k].wait_recv()
            if k % 2 == 0:
                self.far.append(self.pass_on(self.piece((x + 3) % 4, d), 23 + k, self.right_dev))
            self.left[k].wait_recv()
            if k % 2 == 1:
                self.far.append(self.pass_on(self.piece((x + 1) % 4, d), 23 + k, self.left_dev))
        self.cores.append(self.pass_on(blk(c, (x + 3) % 4), 32, self.core_dev))
        self.cores.append(self.pass_on(blk(c, (x + 1) % 4), 33, self.core_dev))

    def far_in(self):
        z, x, c, _ = place()
        for cp in self.far:
            cp.wait_recv()
        self.cores.append(self.pass_on(blk(c, (x + 2) % 4), 34, self.core_dev))

    def cores_in(self):
        for cp in self.cores:
            cp.wait_recv()

    def drain(self):
        for cp in self.sent:
            cp.wait_send()


def add_rows(dst, dst_at, terms, rows, step=32):
    for r in range(0, rows, step):
        total = None
        for ref, base in terms:
            v = ref[pl.ds(base + r, step), :].astype(F32)
            total = v if total is None else total + v
        dst[pl.ds(dst_at + r, step), :] = total.astype(dst.dtype)


class Reduce:
    sems = 4 + 2 + 4 + 7

    @staticmethod
    def scratch():
        return [
            pltpu.VMEM((512, 1024), BF),
            pltpu.VMEM((128, 1024), BF),
            pltpu.VMEM((128, 1024), BF),
            pltpu.VMEM((256, 1024), BF),
            pltpu.VMEM((256, 1024), BF),
            pltpu.VMEM((128, 1024), BF),
            pltpu.VMEM((112, 1024), BF),
        ]

    def __init__(self, part, bufs, ss, rs):
        self.part, self.ss, self.rs = part, ss, rs
        self.crecv, self.obuf, self.orecv, self.nbuf, self.xrecv, self.zbuf, self.zrecv = bufs
        self.sent = []

    def send(self, src, dst, k, dev):
        cp = rcopy(src, dst, self.ss.at[k], self.rs.at[k], dev)
        self.sent.append(cp)
        return cp

    def start_c(self):
        z, x, c, _ = place()
        self.cores = []
        for k, d in enumerate((2, 1, 3, 0)):
            xx = (x + d) % 4
            self.cores.append(
                self.send(
                    self.part.at[blk(1 - c, xx)],
                    self.crecv.at[pl.ds(pl.multiple_of(xx * 128, 128), 128)],
                    k,
                    {"c": 1 - c},
                )
            )

    def start_opposite(self):
        z, x, c, _ = place()
        self.cores[0].wait_recv()
        o = (x + 2) % 4
        terms = [(self.part, c * 512 + o * 128), (self.crecv, o * 128)]
        add_rows(self.obuf, 0, terms, 128)
        half = pl.ds(0, 64)
        rest = pl.ds(64, 64)
        self.o_right = self.send(self.obuf.at[half], self.orecv.at[half], 4, {"x": (x + 1) % 4})
        self.o_left = self.send(self.obuf.at[rest], self.orecv.at[rest], 5, {"x": (x + 3) % 4})

    def start_near(self):
        z, x, c, _ = place()
        r, l = (x + 1) % 4, (x + 3) % 4
        self.near = []
        self.cores[1].wait_recv()
        add_rows(self.nbuf, 64, [(self.part, c * 512 + r * 128 + 64), (self.crecv, r * 128 + 64)], 64)
        s = pl.ds(64, 64)
        self.near.append(self.send(self.nbuf.at[s], self.xrecv.at[s], 6, {"x": r}))
        self.cores[2].wait_recv()
        add_rows(self.nbuf, 128, [(self.part, c * 512 + l * 128), (self.crecv, l * 128)], 64)
        s = pl.ds(128, 64)
        self.near.append(self.send(self.nbuf.at[s], self.xrecv.at[s], 7, {"x": l}))

    def finish_near(self):
        z, x, c, _ = place()
        r, l = (x + 1) % 4, (x + 3) % 4
        self.o_right.wait_recv()
        add_rows(
            self.nbuf, 0,
            [(self.part, c * 512 + r * 128), (self.crecv, r * 128), (self.orecv, 0)], 64,
        )
        s = pl.ds(0, 64)
        self.near.append(self.send(self.nbuf.at[s], self.xrecv.at[s], 8, {"x": r}))
        self.o_left.wait_recv()
        add_rows(
            self.nbuf, 192,
            [(self.part, c * 512 + l * 128 + 64), (self.crecv, l * 128 + 64), (self.orecv, 64)], 64,
        )
        s = pl.ds(192, 64)
        self.near.append(self.send(self.nbuf.at[s], self.xrecv.at[s], 9, {"x": l}))

    def start_z(self):
        z, x, c, _ = place()
        self.cores[3].wait_recv()
        for cp in self.near:
            cp.wait_recv()
        terms = [(self.part, c * 512 + x * 128), (self.crecv, x * 128), (self.xrecv, 0), (self.xrecv, 128)]
        add_rows(self.zbuf, 0, terms, 128)
        self.zc = []
        for d in range(1, 8):
            t = (z + d) % 8
            src = self.zbuf.at[pl.ds(pl.multiple_of(t * 16, 16), 16)]
            self.zc.append(self.send(src, self.zrecv.at[pl.ds((d - 1) * 16, 16)], 9 + d, dev_z(t)))

    def total(self):
        z, x, c, _ = place()
        out = self.zbuf[pl.ds(pl.multiple_of(z * 16, 16), 16), :].astype(F32)
        for d in range(1, 8):
            self.zc[d - 1].wait_recv()
            out = out + self.zrecv[pl.ds((d - 1) * 16, 16), :].astype(F32)
        return out

    def drain(self):
        for cp in self.sent:
            cp.wait_send()


class YGather:
    def __init__(self, own, full, ss, rs):
        self.own, self.full, self.ss, self.rs = own, full, ss, rs

    def copy(self, src, m, h, yy, k, dev):
        return rcopy(src, self.full[m].at[h, yy], self.ss.at[k], self.rs.at[k], dev)

    def start(self):
        y = at("y")
        self.up, self.down = {"y": (y + 1) % 4}, {"y": (y + 3) % 4}
        self.ups, self.downs = {}, {}
        for h in range(2):
            for m in range(2):
                self.ups[h, m] = self.copy(self.own(m, h), m, h, y, h * 2 + m, self.up)
        for h in (1, 0):
            for m in range(2):
                self.downs[h, m] = self.copy(self.own(m, h), m, h, y, 4 + h * 2 + m, self.down)

    def forward(self):
        y = at("y")
        self.far = []
        for m in range(2):
            self.ups[0, m].wait_recv()
            yy = (y + 3) % 4
            self.far.append(self.copy(self.full[m].at[0, yy], m, 0, yy, 8 + m, self.up))
            self.downs[1, m].wait_recv()
            yy = (y + 1) % 4
            self.far.append(self.copy(self.full[m].at[1, yy], m, 1, yy, 10 + m, self.down))

    def finish(self):
        for m in range(2):
            self.ups[1, m].wait_recv()
            self.downs[0, m].wait_recv()
        for cp in self.far:
            cp.wait_recv()

    def drain(self):
        for cp in self.far + list(self.ups.values()) + list(self.downs.values()):
            cp.wait_send()


class YReduce:
    @staticmethod
    def scratch(rows):
        return [
            pltpu.VMEM((2, 2, rows, 512), BF),
            pltpu.VMEM((2, 2, rows, 512), BF),
            pltpu.VMEM((2, 2, 2, rows, 512), BF),
        ]

    def __init__(self, part, rows, bufs, ss, rs):
        self.part, self.rows, self.ss, self.rs = part, rows, ss, rs
        self.orv, self.nh, self.xin = bufs
        y = at("y")
        self.up, self.down = {"y": (y + 1) % 4}, {"y": (y + 3) % 4}
        self.opp, self.plain, self.mixed = {}, [], []

    def copy(self, src, dst, k, dev):
        return rcopy(src, dst, self.ss.at[k], self.rs.at[k], dev)

    def start(self, m):
        y = at("y")
        u, d, o = (y + 1) % 4, (y + 3) % 4, (y + 2) % 4
        self.opp[m, 0] = self.copy(self.part[m].at[0, o], self.orv.at[m, 0], m, self.up)
        self.opp[m, 1] = self.copy(self.part[m].at[1, o], self.orv.at[m, 1], 2 + m, self.down)
        self.plain.append(self.copy(self.part[m].at[1, u], self.xin.at[m, 0, 1], 4 + m, self.up))
        self.plain.append(self.copy(self.part[m].at[0, d], self.xin.at[m, 1, 0], 6 + m, self.down))

    def middle(self, m):
        y = at("y")
        u, d = (y + 1) % 4, (y + 3) % 4
        for h, yy, dev in ((0, u, self.up), (1, d, self.down)):
            self.opp[m, h].wait_recv()
            for s in range(0, self.rows, 32):
                self.nh[m, h, s : s + 32, :] = (
                    self.part[m][h, yy, s : s + 32, :].astype(F32) + self.orv[m, h, s : s + 32, :].astype(F32)
                ).astype(BF)
            self.mixed.append(self.copy(self.nh.at[m, h], self.xin.at[m, h, h], 8 + 2 * h + m, dev))

    def finish(self):
        for cp in self.plain + self.mixed:
            cp.wait_recv()

    def total(self, m, h, rows):
        return (
            self.part[m][h, at("y"), rows, :].astype(F32)
            + self.xin[m, 0, h, rows, :].astype(F32)
            + self.xin[m, 1, h, rows, :].astype(F32)
        )

    def drain(self):
        for cp in list(self.opp.values()) + self.plain + self.mixed:
            cp.wait_send()


def inv_rms(f):
    return lax.rsqrt(jnp.mean(f * f, axis=1, keepdims=True) + norm_eps)


def slot_of(owners, m, k):
    own, rank = owners[m, k], jnp.int32(0)
    for j in range(16):
        rank = rank + jnp.where((owners[m, j] == own) & (j < k), 1, 0)
    return own * 3 + rank


def ones_if(hit):
    return jnp.full((64, 512), jnp.where(hit, 1.0, 0.0), F32).astype(BF)


def half(h):
    return pl.ds(pl.multiple_of(h * 512, 128), 512)


VM = pl.BlockSpec(memory_space=pltpu.VMEM)
SM = pl.BlockSpec(memory_space=pltpu.SMEM)
DMA = pltpu.SemaphoreType.DMA


def comm_call(kernel, name, ident, out_shape, scratch, in_specs, args):
    return pl.pallas_call(
        kernel,
        name=name,
        out_shape=out_shape,
        in_specs=in_specs,
        out_specs=(VM,) * len(out_shape),
        scratch_shapes=scratch,
        compiler_params=pltpu.CompilerParams(collective_id=ident, has_side_effects=True, vmem_limit_bytes=67_043_328),
        cost_estimate=pl.CostEstimate(flops=40_000_000_000, bytes_accessed=2**23, transcendentals=0),
    )(*args)


def shape(*dims, kind=BF):
    return jax.ShapeDtypeStruct(dims, kind)


def before_input(f, inv, gated, base):
    return base + inv * gated - f * inv * inv * inv * jnp.mean(f * gated, axis=1, keepdims=True)


def full(w):
    return w[...].reshape(1024, 512)


def mul(a, b, dims):
    return lax.dot_general(a, b, (dims, ((), ())), preferred_element_type=F32)


def up(rows, src, w_in, hid, act):
    h = mul(src[rows, :], full(w_in), ((1,), (0,)))
    hid[rows, :] = h
    act[rows, :] = gelu_value(h).astype(BF)


def down(rows, cot, w_out, hid, dh):
    d = mul(cot[rows, :], full(w_out), ((1,), (0,)))
    dh[rows, :] = (d * gelu_slope(hid[rows, :])).astype(BF)


def back(rows, src, w, part):
    part[rows, :] = mul(src[rows, :], full(w), ((1,), (1,))).astype(BF)


def outer(left, right, store):
    for i in range(4):
        store(i, mul(left[:, i * 256 : (i + 1) * 256], right[...], ((0,), (0,))).astype(BF))


def as_flat(ref):
    def store(i, v):
        ref[i // 2, (i % 2) * 2] = v[:128]
        ref[i // 2, (i % 2) * 2 + 1] = v[128:]

    return store


def as_tiles(ref):
    def store(i, v):
        ref[i * 4 : (i + 1) * 4] = v.reshape(4, 64, 512)

    return store


def pick_tiles(owners, m, slots, w):
    def tile(k, _):
        want = slot_of(owners, m, k)
        total = jnp.zeros((64, 512), BF)
        for q in range(24):
            r, s = q // 3, q % 3
            total = total + slots[r // 4, r % 4, s * 64 : (s + 1) * 64, :] * ones_if(want == q)
        w[k] = total
        return 0

    lax.fori_loop(0, 16, tile, 0)


def place_tiles(owners, m, g, p):
    dest = [slot_of(owners, m, k) for k in range(16)]

    def slot(q, _):
        row, s = q // 3, q % 3
        total = jnp.zeros((64, 512), BF)
        for k in range(16):
            total = total + g[k] * ones_if(dest[k] == q)
        p[row // 4, row % 4, pl.ds(pl.multiple_of(s * 64, 64), 64), :] = total
        return 0

    lax.fori_loop(0, 24, slot, 0)


def scratch_of():
    vm = pltpu.VMEM
    tok, wt, act, f32 = vm((1024, 1024), BF), vm((2, 4, 128, 512), BF), vm((1024, 512), BF), vm((1024, 512), F32)
    tiles, slots, flat = vm((16, 64, 512), BF), vm((2, 4, 192, 512), BF), vm((64, 8, 512), BF)
    own, n, k = vm((16, 1024), BF), Gather.sems, Reduce.sems
    named = dict(
        normed_one=tok, normed_two=tok, cot_two=tok, cot_one=tok, part_a=tok, part_b=tok,
        w_in_one=wt, w_out_one=wt, w_in_two=tiles, w_out_two=tiles, hid_one=f32, hid_two=f32, act_one=act, act_two=act, dh=act,
        pair=vm((2, 2, 192, 512), BF), rbuf_w=flat, sbuf_w=flat, wide=vm((4, 512, 128), F32), s_in=slots, s_out=slots, gt_in=tiles, gt_out=tiles, p_in=slots, p_out=slots,
        gf_in=wt, gf_out=wt, sbuf_g=flat, tile_sum=vm((2, 2, 192, 512), BF), tile_got=vm((2, 192, 512), BF),
        own_one=own, own_two=own, mid=own, grad_mid=own,
        gs=DMA((4, n)), gr=DMA((4, n)), rs=DMA((4, k)), rr=DMA((4, k)), ys=DMA((4, 12)), yr=DMA((4, 12)),
        ws=DMA((2,)), wr=DMA((2,)), ps=DMA((4,)), pr=DMA((4,)),
    )
    reduces = [Reduce.scratch() for _ in range(3)]
    return named, reduces, YReduce.scratch(192), YReduce.scratch(128)


class Bag:
    pass


def step_kernel(owners, tokens, cot, gains, f_in, f_out, t_in, t_out, hidden_out, grad_tokens, rbuf, tile_grad, *scratch):
    named, reduces, tile_y, flat_y = scratch_of()
    v, refs = Bag(), list(scratch)
    for name in named:
        setattr(v, name, refs.pop(0))
    bufs = []
    for r in reduces:
        bufs.append(refs[: len(r)])
        refs = refs[len(r) :]
    tile_bufs, flat_bufs = refs[:3], refs[3:]
    z, x, c, y = place()
    zh = at("zh")
    near = [blk(c, (x + d) % 4) for d in (0, 3, 1, 2)]
    far = [blk(1 - c, 0, 256), blk(1 - c, 2, 256)]

    def prepare():
        f = tokens[...].astype(F32)
        v.own_one[...] = (f * inv_rms(f) * gains[0:1, :]).astype(BF)
        for m, flat in enumerate((f_in, f_out)):
            for h in range(2):
                for d in range(4):
                    for q in range(4):
                        cols = slice(h * 512 + q * 128, h * 512 + q * 128 + 128)
                        v.wide[q, pl.ds(h * 256 + m * 4 + d, 32, stride=8), :] = flat[d * 32 : (d + 1) * 32, cols].astype(F32)
        for q in range(4):
            sbuf[:, :, q * 128 : (q + 1) * 128] = v.wide[q].reshape(64, 8, 128).astype(BF)

    sbuf = v.sbuf_w
    greet_all(prepare)
    exchange_start(sbuf, v.rbuf_w, v.ws.at[0], v.wr.at[0])
    a = Gather(v.own_one, v.normed_one, v.gs.at[0], v.gr.at[0])
    b = Gather(cot, v.cot_two, v.gs.at[1], v.gr.at[1])
    a.start_z()
    for m, t in enumerate((t_in, t_out)):
        v.pair[m, zh] = t[:, half(zh)]
    exchange_wait(sbuf, v.rbuf_w, v.ws.at[0], v.wr.at[0])
    for h in range(2):
        def tile(q, _):
            got = [v.rbuf_w[h * 32 + q * 4 + i].astype(F32) for i in range(4)]
            rows = pl.ds(pl.multiple_of(q * 16, 16), 16)
            v.w_in_one[h, y, rows, :] = jnp.concatenate([u[0:4] for u in got], axis=0).astype(BF)
            v.w_out_one[h, y, rows, :] = jnp.concatenate([u[4:8] for u in got], axis=0).astype(BF)
            return 0

        lax.fori_loop(0, 8, tile, 0)
    ones = (v.w_in_one, v.w_out_one)
    yg = YGather(lambda m, h: ones[m].at[h, y], ones, v.ys.at[0], v.yr.at[0])
    yg.start()
    a.start_x()
    pairs = [
        rcopy(t.at[:, half(1 - zh)], v.pair.at[m, zh], v.ps.at[m], v.pr.at[m], {"zh": 1 - zh})
        for m, t in enumerate((t_in, t_out))
    ]
    b.start_z()
    yg.forward()
    a.sides_in()
    a.far_in()
    a.cores_in()
    yg.finish()

    for rows in far:
        up(rows, v.normed_one, v.w_in_one, v.hid_one, v.act_one)
        back(rows, v.act_one, v.w_out_one, v.part_a)
    r = Reduce(v.part_a, bufs[0], v.rs.at[0], v.rr.at[0])
    r.start_c()
    for i in range(2):
        rows = blk(c, 2 * i, 256)
        up(rows, v.normed_one, v.w_in_one, v.hid_one, v.act_one)
        back(rows, v.act_one, v.w_out_one, v.part_a)
    r.start_opposite()
    r.start_near()
    slots = (v.s_in, v.s_out)
    for cp in pairs:
        cp.wait_recv()
    yt = YGather(lambda m, h: v.pair.at[m, h], slots, v.ys.at[1], v.yr.at[1])
    yt.start()
    for m in range(2):
        for h in range(2):
            slots[m][h, y] = v.pair[m, h]
    r.finish_near()
    b.start_x()
    r.start_z()
    yt.forward()
    b.sides_in()
    v.mid[...] = (tokens[...].astype(F32) + r.total()).astype(BF)
    f = v.mid[...].astype(F32)
    v.own_two[...] = (f * inv_rms(f) * gains[1:2, :]).astype(BF)
    a2 = Gather(v.own_two, v.normed_two, v.gs.at[2], v.gr.at[2])
    a2.start_z()
    r.drain()
    b.far_in()
    a2.start_x()
    yt.finish()
    pick_tiles(owners, 0, slots[0], v.w_in_two)
    a2.sides_in()
    pick_tiles(owners, 1, slots[1], v.w_out_two)
    b.cores_in()

    def layer_two(rows):
        up(rows, v.normed_two, v.w_in_two, v.hid_two, v.act_two)
        down(rows, v.cot_two, v.w_out_two, v.hid_two, v.dh)
        back(rows, v.dh, v.w_in_two, v.part_a)

    for rows in near[:3]:
        layer_two(rows)
    a2.far_in()
    layer_two(near[3])
    a2.cores_in()
    for rows in far:
        layer_two(rows)
    r = Reduce(v.part_a, bufs[1], v.rs.at[1], v.rr.at[1])
    r.start_c()
    r.start_opposite()
    r.start_near()
    ty = YReduce((v.p_in, v.p_out), 192, tile_bufs, v.ys.at[2], v.yr.at[2])
    outer(v.normed_two, v.dh, as_tiles(v.gt_in))
    place_tiles(owners, 0, v.gt_in, v.p_in)
    ty.start(0)
    r.finish_near()
    outer(v.cot_two, v.act_two, as_tiles(v.gt_out))
    place_tiles(owners, 1, v.gt_out, v.p_out)
    ty.start(1)
    r.start_z()
    for i in range(4):
        back(pl.ds(i * 256, 256), v.act_two, v.w_out_two, v.part_b)
    s = Reduce(v.part_b, bufs[2], v.rs.at[2], v.rr.at[2])
    s.start_c()
    s.start_opposite()
    s.start_near()
    f = v.mid[...].astype(F32)
    v.grad_mid[...] = before_input(f, inv_rms(f), r.total() * gains[1:2, :], cot[...].astype(F32)).astype(BF)
    b2 = Gather(v.grad_mid, v.cot_one, v.gs.at[3], v.gr.at[3])
    b2.start_z()
    r.drain()
    ty.middle(0)
    s.finish_near()
    b2.start_x()
    ty.middle(1)
    s.start_z()
    b2.sides_in()

    def layer_one(rows):
        down(rows, v.cot_one, v.w_out_one, v.hid_one, v.dh)
        back(rows, v.dh, v.w_in_one, v.part_a)

    for rows in near[:3]:
        layer_one(rows)
    b2.far_in()
    layer_one(near[3])
    ty.finish()
    for m in range(2):
        for h in range(2):
            for k in range(0, 192, 32):
                rows = pl.ds(k, 32)
                v.tile_sum[m, h, rows, :] = ty.total(m, h, rows).astype(BF)
    swaps = [
        rcopy(v.tile_sum.at[m, 1 - zh], v.tile_got.at[m], v.ps.at[2 + m], v.pr.at[2 + m], {"zh": 1 - zh})
        for m in range(2)
    ]
    b2.cores_in()
    fy = YReduce((v.gf_in, v.gf_out), 128, flat_bufs, v.ys.at[3], v.yr.at[3])
    outer(v.cot_one, v.act_one, as_flat(v.gf_out))
    fy.start(1)
    for rows in far:
        down(rows, v.cot_one, v.w_out_one, v.hid_one, v.dh)
    for rows in far:
        back(rows, v.dh, v.w_in_one, v.part_a)
    r = Reduce(v.part_a, bufs[0], v.rs.at[3], v.rr.at[3])
    r.start_c()
    outer(v.normed_one, v.dh, as_flat(v.gf_in))
    fy.start(0)
    r.start_opposite()
    r.start_near()
    fy.middle(1)
    r.finish_near()
    fy.middle(0)
    r.start_z()
    fy.finish()
    for h in range(2):
        def tile(q, _):
            rows = pl.ds(pl.multiple_of(q * 16, 16), 16)
            t = [fy.total(m, h, rows) for m in range(2)]
            for i in range(4):
                v.sbuf_g[h * 32 + q * 4 + i] = jnp.concatenate(
                    [t[0][4 * i : 4 * i + 4], t[1][4 * i : 4 * i + 4]], axis=0
                ).astype(BF)
            return 0

        lax.fori_loop(0, 8, tile, 0)
    exchange_start(v.sbuf_g, rbuf, v.ws.at[1], v.wr.at[1])
    for m, cp in enumerate(swaps):
        cp.wait_recv()
        tile_grad[m, :, half(zh)] = v.tile_sum[m, zh]
        tile_grad[m, :, half(1 - zh)] = v.tile_got[m]
    hidden_out[...] = (v.mid[...].astype(F32) + s.total()).astype(BF)
    f = tokens[...].astype(F32)
    grad_tokens[...] = before_input(f, inv_rms(f), r.total() * gains[0:1, :], v.grad_mid[...].astype(F32)).astype(BF)
    exchange_wait(v.sbuf_g, rbuf, v.ws.at[1], v.wr.at[1])
    exchange_sent(v.sbuf_g, v.ws.at[1])
    exchange_sent(sbuf, v.ws.at[0])
    for cp in pairs + swaps:
        cp.wait_send()
    for q in (a, b, a2, b2, yg, yt, ty, fy, r, s):
        q.drain()


def step(*args):
    named, reduces, tile_y, flat_y = scratch_of()
    out = (shape(16, 1024), shape(16, 1024), shape(64, 8, 512), shape(2, 192, 1024))
    scratch = list(named.values()) + sum(reduces, []) + tile_y + flat_y
    return comm_call(step_kernel, "step", 0, out, scratch, [SM] + [VM] * 7, args)


def adam_kernel(
    owners, rbuf, tile_grad, f_in, f_out, fm, fv, t_in, t_out, tm, tv,
    nf_in, nf_out, nfm, nfv, nt_in, nt_out, ntm, ntv, wide,
):
    d = pl.program_id(0)

    @pl.when(d == 0)
    def _():
        for q in range(4):
            wide[q] = rbuf[:, :, q * 128 : (q + 1) * 128].astype(F32).reshape(512, 128)

    row = at("zh") * 4 + at("y")
    for m, (w, nw) in enumerate(((f_in, nf_in), (f_out, nf_out))):
        for h in range(2):
            for q in range(4):
                cols = slice(h * 512 + q * 128, h * 512 + q * 128 + 128)
                grad = wide[q, pl.ds(h * 256 + m * 4 + d, 32, stride=8), :]
                w1, m1, v1 = adam_update(w[:, cols], grad, fm[m, :, cols], fv[m, :, cols])
                nw[:, cols] = w1
                nfm[m, :, cols] = m1
                nfv[m, :, cols] = v1
    for m, (w, nw) in enumerate(((t_in, nt_in), (t_out, nt_out))):
        count = jnp.int32(0)
        for k in range(16):
            count = count + jnp.where(owners[m, k] == row, 1, 0)
        for i in range(3):
            rows = slice(16 * i, 16 * i + 16)
            at_row = lax.broadcasted_iota(jnp.int32, (16, 1024), 0) + (d * 48 + 16 * i)
            keep = at_row < count * 64
            w0, m0, v0 = w[rows, :], tm[m, rows, :], tv[m, rows, :]
            w1, m1, v1 = adam_update(w0, tile_grad[m, rows, :].astype(F32), m0, v0)
            nw[rows, :] = jnp.where(keep, w1.astype(F32), w0.astype(F32)).astype(BF)
            ntm[m, rows, :] = jnp.where(keep, m1, m0)
            ntv[m, rows, :] = jnp.where(keep, v1, v0)


def adam(*args):
    flat = pl.BlockSpec((32, 1024), lambda d: (d, 0))
    tile = pl.BlockSpec((48, 1024), lambda d: (d, 0))
    flats = pl.BlockSpec((2, 32, 1024), lambda d: (0, d, 0))
    tiles = pl.BlockSpec((2, 48, 1024), lambda d: (0, d, 0))
    state = [flat, flat, flats, flats, tile, tile, tiles, tiles]
    return pl.pallas_call(
        adam_kernel,
        name="adam",
        grid=(4,),
        out_shape=(
            shape(128, 1024), shape(128, 1024), shape(2, 128, 1024, kind=F32), shape(2, 128, 1024, kind=F32),
            shape(192, 1024), shape(192, 1024), shape(2, 192, 1024, kind=F32), shape(2, 192, 1024, kind=F32),
        ),
        in_specs=[SM, VM, tiles] + state,
        out_specs=tuple(state),
        scratch_shapes=[pltpu.VMEM((4, 512, 128), F32)],
        cost_estimate=pl.CostEstimate(flops=4_000_000_000, bytes_accessed=13 * 2**20, transcendentals=0),
    )(*args)


def shards(
    tokens, grad_out, gains, flat_in, flat_out, flat_moment, flat_second,
    tile_in, tile_out, tile_moment, tile_second, owners,
):
    own = owners[:, 0, :]
    tile, tiles = (192, 1024), (2, 192, 1024)
    hidden_out, grad_tokens, rbuf, tile_grad = step(
        own, tokens, grad_out, gains, flat_in, flat_out, tile_in.reshape(tile), tile_out.reshape(tile)
    )
    outs = adam(
        own, rbuf, tile_grad, flat_in, flat_out, flat_moment, flat_second,
        tile_in.reshape(tile), tile_out.reshape(tile), tile_moment.reshape(tiles), tile_second.reshape(tiles),
    )
    return (
        hidden_out, grad_tokens, *outs[:4], outs[4].reshape(tile_in.shape), outs[5].reshape(tile_in.shape),
        outs[6].reshape(tile_moment.shape), outs[7].reshape(tile_moment.shape),
    )


def solution(mesh):
    mesh = Mesh(mesh.devices.reshape(2, 4, 4, 4, 2), ALL)
    whole = P(ALL, None)
    state = P(None, ALL, None)
    tile = P(COL, ROW, None, None)
    tile_state = P(None, COL, ROW, None, None)
    return jax.shard_map(
        shards,
        mesh=mesh,
        in_specs=(whole, whole, P(), whole, whole, state, state, tile, tile, tile_state, tile_state, P(None, COL, None)),
        out_specs=(whole, whole, whole, whole, state, state, tile, tile, tile_state, tile_state),
        check_vma=False,
    )
```

```python
import functools

import jax
import jax.numpy as jnp
from jax import lax
from jax.experimental import pallas as pl
from jax.experimental.pallas import tpu as pltpu
from jax.sharding import Mesh, PartitionSpec as P

norm_eps = 1e-06
beta_one = 0.9
beta_two = 0.95
learn_rate = 0.002
decay_rate = 0.1
adam_eps = 1e-08
gelu_coef = 0.7978845608

ALL = ("zh", "y", "zl", "x", "c")
ROW = ("zh", "y")
COL = ("zl", "x", "c")
MESH = pl.DeviceIdType.MESH
BF = jnp.bfloat16
F32 = jnp.float32

def gelu_value(hidden):
    tanh_term = jnp.tanh(gelu_coef * (hidden + 0.044715 * hidden * hidden * hidden))
    return 0.5 * hidden * (1.0 + tanh_term)


def gelu_slope(hidden):
    tanh_term = jnp.tanh(gelu_coef * (hidden + 0.044715 * hidden * hidden * hidden))
    return 0.5 * (1.0 + tanh_term) + 0.5 * hidden * (1.0 - tanh_term * tanh_term) * gelu_coef * (
        1.0 + 0.134145 * hidden * hidden
    )


def adam_update(weight, gradient, moment, second):
    new_moment = beta_one * moment + (1.0 - beta_one) * gradient
    new_second = beta_two * second + (1.0 - beta_two) * gradient * gradient
    weight_float = weight.astype(jnp.float32)
    stepped = weight_float - learn_rate * (
        new_moment / (jnp.sqrt(new_second) + adam_eps) + decay_rate * weight_float
    )
    return (stepped.astype(jnp.bfloat16), new_moment, new_second)


def dev_z(z):
    return {"zh": z // 4, "zl": z % 4}


def at(a):
    return lax.axis_index(a)


def place():
    return at("zh") * 4 + at("zl"), at("x"), at("c"), at("y")


def flat_dev(t):
    return {"zh": t // 32, "zl": (t // 8) % 4, "x": (t // 2) % 4, "c": t % 2}


def my_flat():
    z, x, c, _ = place()
    return z * 8 + x * 2 + c


def greet_all(meanwhile):
    me = my_flat()
    y = at("y")
    sem = pltpu.get_barrier_semaphore()

    def one(o, _):
        pl.semaphore_signal(sem, inc=1, device_id=flat_dev((me + o) % 64), device_id_type=MESH)
        return 0

    lax.fori_loop(1, 64, one, 0)
    for d in (1, 3):
        pl.semaphore_signal(sem, inc=1, device_id={"y": (y + d) % 4}, device_id_type=MESH)
    meanwhile()
    pl.semaphore_wait(sem, 65)


def rcopy(src, dst, ssem, rsem, dev):
    cp = pltpu.make_async_remote_copy(
        src_ref=src, dst_ref=dst, send_sem=ssem, recv_sem=rsem, device_id=dev, device_id_type=MESH
    )
    cp.start()
    return cp


def exchange_start(sbuf, rbuf, ssem, rsem):
    me = my_flat()

    def one(o, _):
        t = (me + o) % 64
        rcopy(sbuf.at[t], rbuf.at[me], ssem, rsem, flat_dev(t))
        return 0

    lax.fori_loop(1, 64, one, 0)
    rbuf[me] = sbuf[me]


def exchange_wait(sbuf, rbuf, ssem, rsem):
    part = pltpu.make_async_copy(rbuf.at[pl.ds(0, 63)], rbuf.at[pl.ds(0, 63)], rsem)
    part.wait()


def exchange_sent(sbuf, ssem):
    part = pltpu.make_async_copy(sbuf.at[pl.ds(0, 63)], sbuf.at[pl.ds(0, 63)], ssem)
    part.wait()


def blk(c, x, n=128, off=0):
    return pl.ds(pl.multiple_of(c * 512 + x * 128 + off, 16), n)


PIECES = (0, 1, 7, 2, 6, 3, 5, 4)


class Gather:
    sems = 7 + 16 + 8 + 4

    def __init__(self, own, full, ss, rs):
        self.own, self.full, self.ss, self.rs = own, full, ss, rs
        z, x, c, _ = place()
        self.right_dev, self.left_dev, self.core_dev = {"x": (x + 1) % 4}, {"x": (x + 3) % 4}, {"c": 1 - c}
        self.right, self.left, self.far, self.cores = [], [], [], []

    def piece(self, xx, d):
        z, x, c, _ = place()
        return blk(c, xx, 16, (z + 8 - d) % 8 * 16)

    def send(self, src, rows, k, dev):
        return rcopy(src, self.full.at[rows], self.ss, self.rs.at[k], dev)

    def pass_on(self, rows, k, dev):
        return self.send(self.full.at[rows], rows, k, dev)

    def start_z(self):
        z, x, c, _ = place()
        mine = self.piece(x, 0)
        self.zc = {d: self.send(self.own, mine, d - 1, dev_z((z + d) % 8)) for d in PIECES[1:]}
        self.right.append(self.send(self.own, mine, 7, self.right_dev))
        self.left.append(self.send(self.own, mine, 15, self.left_dev))
        self.full[mine, :] = self.own[...]

    def start_x(self):
        z, x, c, _ = place()
        for k in range(1, 8):
            d = PIECES[k]
            self.zc[d].wait_recv()
            self.right.append(self.pass_on(self.piece(x, d), 7 + k, self.right_dev))
            self.left.append(self.pass_on(self.piece(x, d), 15 + k, self.left_dev))
        self.cores.append(self.pass_on(blk(c, x), 31, self.core_dev))

    def sides_in(self):
        z, x, c, _ = place()
        for k in range(8):
            d = PIECES[k]
            self.right[k].wait_recv()
            if k % 2 == 0:
                self.far.append(self.pass_on(self.piece((x + 3) % 4, d), 23 + k, self.right_dev))
            self.left[k].wait_recv()
            if k % 2 == 1:
                self.far.append(self.pass_on(self.piece((x + 1) % 4, d), 23 + k, self.left_dev))
        self.cores.append(self.pass_on(blk(c, (x + 3) % 4), 32, self.core_dev))
        self.cores.append(self.pass_on(blk(c, (x + 1) % 4), 33, self.core_dev))

    def far_in(self):
        z, x, c, _ = place()
        for cp in self.far:
            cp.wait_recv()
        self.cores.append(self.pass_on(blk(c, (x + 2) % 4), 34, self.core_dev))

    def cores_in(self):
        for cp in self.cores:
            cp.wait_recv()

    def drain(self):
        sent_rows(self.full, self.ss)


def sent_rows(ref, sem):
    rows = ref.at[pl.ds(0, 1008)]
    pltpu.make_async_copy(rows, rows, sem).wait()


def add_rows(dst, dst_at, terms, rows, step=32):
    for r in range(0, rows, step):
        total = None
        for ref, base in terms:
            v = ref[pl.ds(base + r, step), :].astype(F32)
            total = v if total is None else total + v
        dst[pl.ds(dst_at + r, step), :] = total.astype(dst.dtype)


class Reduce:
    sems = 4 + 2 + 4 + 7

    @staticmethod
    def scratch():
        return [
            pltpu.VMEM((512, 1024), BF),
            pltpu.VMEM((128, 1024), BF),
            pltpu.VMEM((128, 1024), BF),
            pltpu.VMEM((256, 1024), BF),
            pltpu.VMEM((256, 1024), BF),
            pltpu.VMEM((128, 1024), BF),
            pltpu.VMEM((112, 1024), BF),
        ]

    def __init__(self, part, bufs, ss, rs):
        self.part, self.ss, self.rs = part, ss, rs
        self.crecv, self.obuf, self.orecv, self.nbuf, self.xrecv, self.zbuf, self.zrecv = bufs

    def send(self, src, dst, k, dev):
        return rcopy(src, dst, self.ss, self.rs.at[k], dev)

    def start_c(self):
        z, x, c, _ = place()
        self.cores = []
        for k, d in enumerate((2, 1, 3, 0)):
            xx = (x + d) % 4
            self.cores.append(
                self.send(
                    self.part.at[blk(1 - c, xx)],
                    self.crecv.at[pl.ds(pl.multiple_of(xx * 128, 128), 128)],
                    k,
                    {"c": 1 - c},
                )
            )

    def start_opposite(self):
        z, x, c, _ = place()
        self.cores[0].wait_recv()
        o = (x + 2) % 4
        terms = [(self.part, c * 512 + o * 128), (self.crecv, o * 128)]
        add_rows(self.obuf, 0, terms, 128)
        half = pl.ds(0, 64)
        rest = pl.ds(64, 64)
        self.o_right = self.send(self.obuf.at[half], self.orecv.at[half], 4, {"x": (x + 1) % 4})
        self.o_left = self.send(self.obuf.at[rest], self.orecv.at[rest], 5, {"x": (x + 3) % 4})

    def start_near(self):
        z, x, c, _ = place()
        r, l = (x + 1) % 4, (x + 3) % 4
        self.near = []
        self.cores[1].wait_recv()
        add_rows(self.nbuf, 64, [(self.part, c * 512 + r * 128 + 64), (self.crecv, r * 128 + 64)], 64)
        s = pl.ds(64, 64)
        self.near.append(self.send(self.nbuf.at[s], self.xrecv.at[s], 6, {"x": r}))
        self.cores[2].wait_recv()
        add_rows(self.nbuf, 128, [(self.part, c * 512 + l * 128), (self.crecv, l * 128)], 64)
        s = pl.ds(128, 64)
        self.near.append(self.send(self.nbuf.at[s], self.xrecv.at[s], 7, {"x": l}))

    def finish_near(self):
        z, x, c, _ = place()
        r, l = (x + 1) % 4, (x + 3) % 4
        self.o_right.wait_recv()
        add_rows(
            self.nbuf, 0,
            [(self.part, c * 512 + r * 128), (self.crecv, r * 128), (self.orecv, 0)], 64,
        )
        s = pl.ds(0, 64)
        self.near.append(self.send(self.nbuf.at[s], self.xrecv.at[s], 8, {"x": r}))
        self.o_left.wait_recv()
        add_rows(
            self.nbuf, 192,
            [(self.part, c * 512 + l * 128 + 64), (self.crecv, l * 128 + 64), (self.orecv, 64)], 64,
        )
        s = pl.ds(192, 64)
        self.near.append(self.send(self.nbuf.at[s], self.xrecv.at[s], 9, {"x": l}))

    def start_z(self):
        z, x, c, _ = place()
        self.cores[3].wait_recv()
        for cp in self.near:
            cp.wait_recv()
        terms = [(self.part, c * 512 + x * 128), (self.crecv, x * 128), (self.xrecv, 0), (self.xrecv, 128)]
        add_rows(self.zbuf, 0, terms, 128)
        self.zc = []
        for d in range(1, 8):
            t = (z + d) % 8
            src = self.zbuf.at[pl.ds(pl.multiple_of(t * 16, 16), 16)]
            self.zc.append(self.send(src, self.zrecv.at[pl.ds((d - 1) * 16, 16)], 9 + d, dev_z(t)))

    def total(self):
        z, x, c, _ = place()
        out = self.zbuf[pl.ds(pl.multiple_of(z * 16, 16), 16), :].astype(F32)
        for d in range(1, 8):
            self.zc[d - 1].wait_recv()
            out = out + self.zrecv[pl.ds((d - 1) * 16, 16), :].astype(F32)
        return out

    def drain(self):
        sent_rows(self.part, self.ss)


class YGather:
    def __init__(self, own, full, ss, rs):
        self.own, self.full, self.ss, self.rs = own, full, ss, rs

    def copy(self, src, m, h, yy, k, dev):
        return rcopy(src, self.full[m].at[h, yy], self.ss.at[k], self.rs.at[k], dev)

    def start(self):
        y = at("y")
        self.up, self.down = {"y": (y + 1) % 4}, {"y": (y + 3) % 4}
        self.ups, self.downs = {}, {}
        for h in range(2):
            for m in range(2):
                self.ups[h, m] = self.copy(self.own(m, h), m, h, y, h * 2 + m, self.up)
        for h in (1, 0):
            for m in range(2):
                self.downs[h, m] = self.copy(self.own(m, h), m, h, y, 4 + h * 2 + m, self.down)

    def forward(self):
        y = at("y")
        self.far = []
        for m in range(2):
            self.ups[0, m].wait_recv()
            yy = (y + 3) % 4
            self.far.append(self.copy(self.full[m].at[0, yy], m, 0, yy, 8 + m, self.up))
            self.downs[1, m].wait_recv()
            yy = (y + 1) % 4
            self.far.append(self.copy(self.full[m].at[1, yy], m, 1, yy, 10 + m, self.down))

    def sides(self):
        for m in range(2):
            self.ups[1, m].wait_recv()
            self.downs[0, m].wait_recv()

    def finish(self):
        for cp in self.far:
            cp.wait_recv()

    def drain(self):
        for cp in self.far + list(self.ups.values()) + list(self.downs.values()):
            cp.wait_send()


class YReduce:
    @staticmethod
    def scratch(rows):
        return [
            pltpu.VMEM((2, 2, rows, 512), BF),
            pltpu.VMEM((2, 2, rows, 512), BF),
            pltpu.VMEM((2, 2, 2, rows, 512), BF),
        ]

    def __init__(self, part, rows, bufs, ss, rs):
        self.part, self.rows, self.ss, self.rs = part, rows, ss, rs
        self.orv, self.nh, self.xin = bufs
        y = at("y")
        self.up, self.down = {"y": (y + 1) % 4}, {"y": (y + 3) % 4}
        self.opp, self.plain, self.mixed = {}, [], []

    def copy(self, src, dst, k, dev):
        return rcopy(src, dst, self.ss.at[k], self.rs.at[k], dev)

    def start(self, m):
        y = at("y")
        u, d, o = (y + 1) % 4, (y + 3) % 4, (y + 2) % 4
        self.opp[m, 0] = self.copy(self.part[m].at[0, o], self.orv.at[m, 0], m, self.up)
        self.opp[m, 1] = self.copy(self.part[m].at[1, o], self.orv.at[m, 1], 2 + m, self.down)
        self.plain.append(self.copy(self.part[m].at[1, u], self.xin.at[m, 0, 1], 4 + m, self.up))
        self.plain.append(self.copy(self.part[m].at[0, d], self.xin.at[m, 1, 0], 6 + m, self.down))

    def middle(self, m):
        y = at("y")
        u, d = (y + 1) % 4, (y + 3) % 4
        for h, yy, dev in ((0, u, self.up), (1, d, self.down)):
            self.opp[m, h].wait_recv()
            for s in range(0, self.rows, 32):
                self.nh[m, h, s : s + 32, :] = (
                    self.part[m][h, yy, s : s + 32, :].astype(F32) + self.orv[m, h, s : s + 32, :].astype(F32)
                ).astype(BF)
            self.mixed.append(self.copy(self.nh.at[m, h], self.xin.at[m, h, h], 8 + 2 * h + m, dev))

    def finish(self):
        for cp in self.plain + self.mixed:
            cp.wait_recv()

    def total(self, m, h, rows):
        return (
            self.part[m][h, at("y"), rows, :].astype(F32)
            + self.xin[m, 0, h, rows, :].astype(F32)
            + self.xin[m, 1, h, rows, :].astype(F32)
        )

    def drain(self):
        for cp in list(self.opp.values()) + self.plain + self.mixed:
            cp.wait_send()


def inv_rms(f):
    return lax.rsqrt(jnp.mean(f * f, axis=1, keepdims=True) + norm_eps)


def slot_of(owners, m, k):
    own, rank = owners[m, k], jnp.int32(0)
    for j in range(16):
        rank = rank + jnp.where((owners[m, j] == own) & (j < k), 1, 0)
    return own * 3 + rank


def ones_if(hit):
    return jnp.full((64, 512), jnp.where(hit, 1.0, 0.0), F32).astype(BF)


def half(h):
    return pl.ds(pl.multiple_of(h * 512, 128), 512)


VM = pl.BlockSpec(memory_space=pltpu.VMEM)
SM = pl.BlockSpec(memory_space=pltpu.SMEM)
DMA = pltpu.SemaphoreType.DMA


def comm_call(kernel, name, ident, out_shape, scratch, in_specs, args):
    return pl.pallas_call(
        kernel,
        name=name,
        out_shape=out_shape,
        in_specs=in_specs,
        out_specs=(VM,) * len(out_shape),
        scratch_shapes=scratch,
        compiler_params=pltpu.CompilerParams(collective_id=ident, has_side_effects=True, vmem_limit_bytes=67_043_328),
        cost_estimate=pl.CostEstimate(flops=40_000_000_000, bytes_accessed=2**23, transcendentals=0),
    )(*args)


def shape(*dims, kind=BF):
    return jax.ShapeDtypeStruct(dims, kind)


def before_input(f, inv, gated, base):
    return base + inv * gated - f * inv * inv * inv * jnp.mean(f * gated, axis=1, keepdims=True)


def full(w):
    return w[...].reshape(1024, 512)


def mul(a, b, dims):
    return lax.dot_general(a, b, (dims, ((), ())), preferred_element_type=F32)


def up(rows, src, w_in, hid, act):
    h = mul(src[rows, :], full(w_in), ((1,), (0,)))
    hid[rows, :] = h
    act[rows, :] = gelu_value(h).astype(BF)


def down(rows, cot, w_out, hid, dh):
    d = mul(cot[rows, :], full(w_out), ((1,), (0,)))
    dh[rows, :] = (d * gelu_slope(hid[rows, :])).astype(BF)


def back(rows, src, w, part):
    part[rows, :] = mul(src[rows, :], full(w), ((1,), (1,))).astype(BF)


def outer(left, right, store):
    for i in range(4):
        store(i, mul(left[:, i * 256 : (i + 1) * 256], right[...], ((0,), (0,))).astype(BF))


def as_flat(ref):
    def store(i, v):
        ref[i // 2, (i % 2) * 2] = v[:128]
        ref[i // 2, (i % 2) * 2 + 1] = v[128:]

    return store


def as_tiles(ref):
    def store(i, v):
        ref[i * 4 : (i + 1) * 4] = v.reshape(4, 64, 512)

    return store


def pick_tiles(owners, slots, weights, yy, first=False):
    for m in range(2):
        def tile(k, _, m=m):
            want = slot_of(owners, m, k)
            total = jnp.zeros((64, 512), BF) if first else weights[m][k]
            for h in range(2):
                for s in range(3):
                    total = total + slots[m][h, yy, s * 64 : (s + 1) * 64, :] * ones_if(want == (h * 4 + yy) * 3 + s)
            weights[m][k] = total
            return 0

        lax.fori_loop(0, 16, tile, 0)


def place_tiles(owners, m, g, p):
    dest = [slot_of(owners, m, k) for k in range(16)]

    def slot(q, _):
        row, s = q // 3, q % 3
        total = jnp.zeros((64, 512), BF)
        for k in range(16):
            total = total + g[k] * ones_if(dest[k] == q)
        p[row // 4, row % 4, pl.ds(pl.multiple_of(s * 64, 64), 64), :] = total
        return 0

    lax.fori_loop(0, 24, slot, 0)


def scratch_of():
    vm = pltpu.VMEM
    tok, wt, act, f32 = vm((1024, 1024), BF), vm((2, 4, 128, 512), BF), vm((1024, 512), BF), vm((1024, 512), F32)
    tiles, slots, flat = vm((16, 64, 512), BF), vm((2, 4, 192, 512), BF), vm((64, 8, 512), BF)
    own, n, k = vm((16, 1024), BF), Gather.sems, Reduce.sems
    named = dict(
        normed_one=tok, normed_two=tok, cot_two=tok, cot_one=tok, part_a=tok, part_b=tok,
        w_in_one=wt, w_out_one=wt, w_in_two=tiles, w_out_two=tiles, hid_one=f32, hid_two=f32, act_one=act, act_two=act, dh=act,
        pair=vm((2, 2, 192, 512), BF), rbuf_w=flat, sbuf_w=flat, wide=vm((4, 512, 128), F32), s_in=slots, s_out=slots, gt_in=tiles, gt_out=tiles, p_in=slots, p_out=slots,
        gf_in=wt, gf_out=wt, sbuf_g=flat, tile_sum=vm((2, 2, 192, 512), BF), tile_got=vm((2, 192, 512), BF),
        own_one=own, own_two=own, mid=own, grad_mid=own,
        gs=DMA((4,)), gr=DMA((4, n)), rs=DMA((4,)), rr=DMA((4, k)), ys=DMA((4, 12)), yr=DMA((4, 12)),
        ws=DMA((2,)), wr=DMA((2,)), ps=DMA((4,)), pr=DMA((4,)),
    )
    reduces = [Reduce.scratch() for _ in range(3)]
    return named, reduces, YReduce.scratch(192), YReduce.scratch(128)


class Bag:
    pass


def step_kernel(owners, tokens, cot, gains, f_in, f_out, t_in, t_out, hidden_out, grad_tokens, rbuf, tile_grad, *scratch):
    named, reduces, tile_y, flat_y = scratch_of()
    v, refs = Bag(), list(scratch)
    for name in named:
        setattr(v, name, refs.pop(0))
    bufs = []
    for r in reduces:
        bufs.append(refs[: len(r)])
        refs = refs[len(r) :]
    tile_bufs, flat_bufs = refs[:3], refs[3:]
    z, x, c, y = place()
    zh = at("zh")
    near = [blk(c, (x + d) % 4) for d in (0, 3, 1, 2)]
    far = [blk(1 - c, 0, 256), blk(1 - c, 2, 256)]

    def prepare():
        f = tokens[...].astype(F32)
        v.own_one[...] = (f * inv_rms(f) * gains[0:1, :]).astype(BF)
        for m, flat in enumerate((f_in, f_out)):
            for h in range(2):
                for d in range(4):
                    for q in range(4):
                        cols = slice(h * 512 + q * 128, h * 512 + q * 128 + 128)
                        v.wide[q, pl.ds(h * 256 + m * 4 + d, 32, stride=8), :] = flat[d * 32 : (d + 1) * 32, cols].astype(F32)
        for q in range(4):
            sbuf[:, :, q * 128 : (q + 1) * 128] = v.wide[q].reshape(64, 8, 128).astype(BF)

    sbuf = v.sbuf_w
    greet_all(prepare)
    exchange_start(sbuf, v.rbuf_w, v.ws.at[0], v.wr.at[0])
    a = Gather(v.own_one, v.normed_one, v.gs.at[0], v.gr.at[0])
    b = Gather(cot, v.cot_two, v.gs.at[1], v.gr.at[1])
    a.start_z()
    for m, t in enumerate((t_in, t_out)):
        v.pair[m, zh] = t[:, half(zh)]
    exchange_wait(sbuf, v.rbuf_w, v.ws.at[0], v.wr.at[0])
    for h in range(2):
        def tile(q, _):
            got = [v.rbuf_w[h * 32 + q * 4 + i].astype(F32) for i in range(4)]
            rows = pl.ds(pl.multiple_of(q * 16, 16), 16)
            v.w_in_one[h, y, rows, :] = jnp.concatenate([u[0:4] for u in got], axis=0).astype(BF)
            v.w_out_one[h, y, rows, :] = jnp.concatenate([u[4:8] for u in got], axis=0).astype(BF)
            return 0

        lax.fori_loop(0, 8, tile, 0)
    ones = (v.w_in_one, v.w_out_one)
    yg = YGather(lambda m, h: ones[m].at[h, y], ones, v.ys.at[0], v.yr.at[0])
    yg.start()
    a.start_x()
    pairs = [
        rcopy(t.at[:, half(1 - zh)], v.pair.at[m, zh], v.ps.at[m], v.pr.at[m], {"zh": 1 - zh})
        for m, t in enumerate((t_in, t_out))
    ]
    b.start_z()
    yg.forward()
    a.sides_in()
    a.far_in()
    a.cores_in()
    yg.sides()
    yg.finish()

    for rows in far:
        up(rows, v.normed_one, v.w_in_one, v.hid_one, v.act_one)
        back(rows, v.act_one, v.w_out_one, v.part_a)
    r = Reduce(v.part_a, bufs[0], v.rs.at[0], v.rr.at[0])
    r.start_c()
    for i in range(2):
        rows = blk(c, 2 * i, 256)
        up(rows, v.normed_one, v.w_in_one, v.hid_one, v.act_one)
        back(rows, v.act_one, v.w_out_one, v.part_a)
    r.start_opposite()
    r.start_near()
    slots = (v.s_in, v.s_out)
    for cp in pairs:
        cp.wait_recv()
    yt = YGather(lambda m, h: v.pair.at[m, h], slots, v.ys.at[1], v.yr.at[1])
    yt.start()
    for m in range(2):
        for h in range(2):
            slots[m][h, y] = v.pair[m, h]
    r.finish_near()
    b.start_x()
    r.start_z()
    yt.forward()
    b.sides_in()
    twos = (v.w_in_two, v.w_out_two)
    pick_tiles(owners, slots, twos, y, True)
    v.mid[...] = (tokens[...].astype(F32) + r.total()).astype(BF)
    f = v.mid[...].astype(F32)
    v.own_two[...] = (f * inv_rms(f) * gains[1:2, :]).astype(BF)
    a2 = Gather(v.own_two, v.normed_two, v.gs.at[2], v.gr.at[2])
    a2.start_z()
    r.drain()
    b.far_in()
    a2.start_x()
    yt.sides()
    pick_tiles(owners, slots, twos, (y + 1) % 4)
    pick_tiles(owners, slots, twos, (y + 3) % 4)
    a2.sides_in()
    yt.finish()
    pick_tiles(owners, slots, twos, (y + 2) % 4)
    b.cores_in()

    def layer_two(rows):
        up(rows, v.normed_two, v.w_in_two, v.hid_two, v.act_two)
        down(rows, v.cot_two, v.w_out_two, v.hid_two, v.dh)
        back(rows, v.dh, v.w_in_two, v.part_a)

    for rows in near[:3]:
        layer_two(rows)
    a2.far_in()
    layer_two(near[3])
    a2.cores_in()
    for rows in far:
        layer_two(rows)
    r = Reduce(v.part_a, bufs[1], v.rs.at[1], v.rr.at[1])
    r.start_c()
    r.start_opposite()
    r.start_near()
    ty = YReduce((v.p_in, v.p_out), 192, tile_bufs, v.ys.at[2], v.yr.at[2])
    outer(v.normed_two, v.dh, as_tiles(v.gt_in))
    place_tiles(owners, 0, v.gt_in, v.p_in)
    ty.start(0)
    r.finish_near()
    outer(v.cot_two, v.act_two, as_tiles(v.gt_out))
    place_tiles(owners, 1, v.gt_out, v.p_out)
    ty.start(1)
    r.start_z()
    for i in range(4):
        back(pl.ds(i * 256, 256), v.act_two, v.w_out_two, v.part_b)
    s = Reduce(v.part_b, bufs[2], v.rs.at[2], v.rr.at[2])
    s.start_c()
    s.start_opposite()
    s.start_near()
    f = v.mid[...].astype(F32)
    v.grad_mid[...] = before_input(f, inv_rms(f), r.total() * gains[1:2, :], cot[...].astype(F32)).astype(BF)
    b2 = Gather(v.grad_mid, v.cot_one, v.gs.at[3], v.gr.at[3])
    b2.start_z()
    r.drain()
    ty.middle(0)
    s.finish_near()
    b2.start_x()
    ty.middle(1)
    s.start_z()
    b2.sides_in()

    def layer_one(rows):
        down(rows, v.cot_one, v.w_out_one, v.hid_one, v.dh)
        back(rows, v.dh, v.w_in_one, v.part_a)

    for rows in near[:3]:
        layer_one(rows)
    b2.far_in()
    layer_one(near[3])
    ty.finish()
    for m in range(2):
        for h in range(2):
            for k in range(0, 192, 32):
                rows = pl.ds(k, 32)
                v.tile_sum[m, h, rows, :] = ty.total(m, h, rows).astype(BF)
    swaps = [
        rcopy(v.tile_sum.at[m, 1 - zh], v.tile_got.at[m], v.ps.at[2 + m], v.pr.at[2 + m], {"zh": 1 - zh})
        for m in range(2)
    ]
    b2.cores_in()
    fy = YReduce((v.gf_in, v.gf_out), 128, flat_bufs, v.ys.at[3], v.yr.at[3])
    outer(v.cot_one, v.act_one, as_flat(v.gf_out))
    fy.start(1)
    for rows in far:
        down(rows, v.cot_one, v.w_out_one, v.hid_one, v.dh)
    for rows in far:
        back(rows, v.dh, v.w_in_one, v.part_a)
    r = Reduce(v.part_a, bufs[0], v.rs.at[3], v.rr.at[3])
    r.start_c()
    outer(v.normed_one, v.dh, as_flat(v.gf_in))
    fy.start(0)
    r.start_opposite()
    r.start_near()
    fy.middle(1)
    r.finish_near()
    fy.middle(0)
    r.start_z()
    fy.finish()
    for h in range(2):
        def tile(q, _):
            rows = pl.ds(pl.multiple_of(q * 16, 16), 16)
            t = [fy.total(m, h, rows) for m in range(2)]
            for i in range(4):
                v.sbuf_g[h * 32 + q * 4 + i] = jnp.concatenate(
                    [t[0][4 * i : 4 * i + 4], t[1][4 * i : 4 * i + 4]], axis=0
                ).astype(BF)
            return 0

        lax.fori_loop(0, 8, tile, 0)
    exchange_start(v.sbuf_g, rbuf, v.ws.at[1], v.wr.at[1])
    for m, cp in enumerate(swaps):
        cp.wait_recv()
        tile_grad[m, :, half(zh)] = v.tile_sum[m, zh]
        tile_grad[m, :, half(1 - zh)] = v.tile_got[m]
    hidden_out[...] = (v.mid[...].astype(F32) + s.total()).astype(BF)
    f = tokens[...].astype(F32)
    grad_tokens[...] = before_input(f, inv_rms(f), r.total() * gains[0:1, :], v.grad_mid[...].astype(F32)).astype(BF)
    exchange_wait(v.sbuf_g, rbuf, v.ws.at[1], v.wr.at[1])
    exchange_sent(v.sbuf_g, v.ws.at[1])
    exchange_sent(sbuf, v.ws.at[0])
    for cp in pairs + swaps:
        cp.wait_send()
    for q in (a, b, a2, b2, yg, yt, ty, fy, r, s):
        q.drain()


def step(*args):
    named, reduces, tile_y, flat_y = scratch_of()
    out = (shape(16, 1024), shape(16, 1024), shape(64, 8, 512), shape(2, 192, 1024))
    scratch = list(named.values()) + sum(reduces, []) + tile_y + flat_y
    return comm_call(step_kernel, "step", 0, out, scratch, [SM] + [VM] * 7, args)


def adam_kernel(
    owners, rbuf, tile_grad, f_in, f_out, fm, fv, t_in, t_out, tm, tv,
    nf_in, nf_out, nfm, nfv, nt_in, nt_out, ntm, ntv, wide,
):
    d = pl.program_id(0)

    @pl.when(d == 0)
    def _():
        for q in range(4):
            wide[q] = rbuf[:, :, q * 128 : (q + 1) * 128].astype(F32).reshape(512, 128)

    row = at("zh") * 4 + at("y")
    for m, (w, nw) in enumerate(((f_in, nf_in), (f_out, nf_out))):
        for h in range(2):
            for q in range(4):
                cols = slice(h * 512 + q * 128, h * 512 + q * 128 + 128)
                grad = wide[q, pl.ds(h * 256 + m * 4 + d, 32, stride=8), :]
                w1, m1, v1 = adam_update(w[:, cols], grad, fm[m, :, cols], fv[m, :, cols])
                nw[:, cols] = w1
                nfm[m, :, cols] = m1
                nfv[m, :, cols] = v1
    for m, (w, nw) in enumerate(((t_in, nt_in), (t_out, nt_out))):
        count = jnp.int32(0)
        for k in range(16):
            count = count + jnp.where(owners[m, k] == row, 1, 0)
        for i in range(3):
            rows = slice(16 * i, 16 * i + 16)
            at_row = lax.broadcasted_iota(jnp.int32, (16, 1024), 0) + (d * 48 + 16 * i)
            keep = at_row < count * 64
            w0, m0, v0 = w[rows, :], tm[m, rows, :], tv[m, rows, :]
            w1, m1, v1 = adam_update(w0, tile_grad[m, rows, :].astype(F32), m0, v0)
            nw[rows, :] = jnp.where(keep, w1.astype(F32), w0.astype(F32)).astype(BF)
            ntm[m, rows, :] = jnp.where(keep, m1, m0)
            ntv[m, rows, :] = jnp.where(keep, v1, v0)


def adam(*args):
    flat = pl.BlockSpec((32, 1024), lambda d: (d, 0))
    tile = pl.BlockSpec((48, 1024), lambda d: (d, 0))
    flats = pl.BlockSpec((2, 32, 1024), lambda d: (0, d, 0))
    tiles = pl.BlockSpec((2, 48, 1024), lambda d: (0, d, 0))
    state = [flat, flat, flats, flats, tile, tile, tiles, tiles]
    return pl.pallas_call(
        adam_kernel,
        name="adam",
        grid=(4,),
        out_shape=(
            shape(128, 1024), shape(128, 1024), shape(2, 128, 1024, kind=F32), shape(2, 128, 1024, kind=F32),
            shape(192, 1024), shape(192, 1024), shape(2, 192, 1024, kind=F32), shape(2, 192, 1024, kind=F32),
        ),
        in_specs=[SM, VM, tiles] + state,
        out_specs=tuple(state),
        scratch_shapes=[pltpu.VMEM((4, 512, 128), F32)],
        cost_estimate=pl.CostEstimate(flops=4_000_000_000, bytes_accessed=13 * 2**20, transcendentals=0),
    )(*args)


def shards(
    tokens, grad_out, gains, flat_in, flat_out, flat_moment, flat_second,
    tile_in, tile_out, tile_moment, tile_second, owners,
):
    own = owners[:, 0, :]
    tile, tiles = (192, 1024), (2, 192, 1024)
    hidden_out, grad_tokens, rbuf, tile_grad = step(
        own, tokens, grad_out, gains, flat_in, flat_out, tile_in.reshape(tile), tile_out.reshape(tile)
    )
    outs = adam(
        own, rbuf, tile_grad, flat_in, flat_out, flat_moment, flat_second,
        tile_in.reshape(tile), tile_out.reshape(tile), tile_moment.reshape(tiles), tile_second.reshape(tiles),
    )
    return (
        hidden_out, grad_tokens, *outs[:4], outs[4].reshape(tile_in.shape), outs[5].reshape(tile_in.shape),
        outs[6].reshape(tile_moment.shape), outs[7].reshape(tile_moment.shape),
    )


def solution(mesh):
    mesh = Mesh(mesh.devices.reshape(2, 4, 4, 4, 2), ALL)
    whole = P(ALL, None)
    state = P(None, ALL, None)
    tile = P(COL, ROW, None, None)
    tile_state = P(None, COL, ROW, None, None)
    return jax.shard_map(
        shards,
        mesh=mesh,
        in_specs=(whole, whole, P(), whole, whole, state, state, tile, tile, tile_state, tile_state, P(None, COL, None)),
        out_specs=(whole, whole, whole, whole, state, state, tile, tile, tile_state, tile_state),
        check_vma=False,
    )
```
